128 devices in a mesh: row: 32 (over y, x, core), col: 4 (over z).
Axes of the slice: x: 4, y: 4, z: 4, core: 2. Of those that a mesh axis runs over, the one named last changes fastest.
Arguments:
- stiff_bb: bfloat16 [384, 3, 128, 384], P(('row', 'col')), may hold values from -6 to 6
- stiff_bi: bfloat16 [384, 384, 3072], P(('row', 'col')), may hold values from -6 to 6
- constraint_modes: bfloat16 [384, 3072, 384], P(('row', 'col')), may hold values from -0.109375 to 0.109375
- interior_mass: float32 [384, 3072], P(('row', 'col')), may hold values from 0.25 to 4
- fixed_modes: bfloat16 [384, 3072, 256], P(('row', 'col')), may hold values from -6 to 6
- mass_bb: bfloat16 [384, 3, 128, 384], P(('row', 'col')), may hold values from -6 to 6
- boundary_map: int32 [384, 3], P(('row', 'col')), may hold values from 0 to 767, as said below
Outputs:
- interface_stiffness: float32 [768, 4, 128, 128], P('row', None, 'col')
- interface_mass: float32 [768, 4, 128, 128], P('row', None, 'col')
- mass_coupling: float32 [384, 256, 384], P(('row', 'col'))
The draws below stay inside these ranges and needn't reach their ends.
Inputs may be any that keep to these rules, and one draw needn't show every extreme that they name: `boundary_map`: row s holds blocks b, b + a, b + c with 0 < a < c < 4, all three in the range of one owner (block // 24). Rows come in aligned row groups of 12; no owner serves more than 1 row of one row group, and in every draw one owner serves exactly 1 row of every row group.
All inputs are finite; a program needn't handle non-finite values.
Results may differ from the reference program's by a relative error of at most 0.0029.
Values sent between devices are 32-bit elements; how exact they have to be, the bound alone decides.
A program may use at most 192 MiB of HBM per device.

```python
import math
import jax
import jax.numpy as jnp
from jax import lax

NI = 3072
BLK = 128
NB = 384
NM = 256
BAND = 4
BPO = 24
SE_GRP = 12
CAP = 1
SETOT = 384
NBLOCK = 768
N_ROW = 32


def draw_boundary_map(key, part):
    slot_count = N_ROW * CAP
    keys = jax.random.split(jax.random.fold_in(key, 17), 7)
    priority_tiers = jax.random.randint(keys[0], (N_ROW,), 0, 4)
    busiest_targets = jax.random.randint(keys[1], (), 0, N_ROW)
    position_owner = jnp.arange(slot_count) // CAP
    random_jitter = jax.random.randint(keys[2], (N_ROW, slot_count), 0, 65536)
    extra_credit = jnp.where(position_owner == busiest_targets, 1 << 20, 0)
    ranking_values = random_jitter + priority_tiers[position_owner][None, :] * 16384 + extra_credit[None, :]
    ranking_values = ranking_values * slot_count + jnp.arange(slot_count)[None, :]
    picked = lax.top_k(ranking_values, SE_GRP)[1]
    order_scores = jax.random.randint(keys[3], (N_ROW, SE_GRP), 0, 4096) * SE_GRP + jnp.arange(SE_GRP)[None, :]
    order = lax.top_k(order_scores, SE_GRP)[1]
    picked = jnp.take_along_axis(picked, order, axis=1)
    owners = (picked // CAP).reshape(SETOT)
    first = jax.random.randint(keys[4], (SETOT,), 1, BAND - 1)
    second = first + jax.random.randint(keys[5], (SETOT,), 1, BAND - first)
    start = owners * BPO + jax.random.randint(keys[6], (SETOT,), 0, BPO - second)
    return jnp.stack([start, start + first, start + second], axis=1).astype(jnp.int32)


def steps_of(rng, extent, cuts, low, top_value):
    gain, own = 1.0, jax.random.fold_in(rng, 6)
    for position, blocks in cuts:
        steps = jnp.exp(jax.random.uniform(jax.random.fold_in(own, position), (blocks,), jnp.float32, low / len(cuts), top_value / len(cuts)))
        gain = gain * jnp.repeat(steps, extent[position] // blocks).reshape([-1 if axis == position else 1 for axis in range(len(extent))])
    return gain


def centred(key, extent, deviation, most, pieces=(), dtype=jnp.bfloat16):
    array = deviation * jax.random.normal(key, extent, jnp.float32)
    if pieces:
        array = array * steps_of(key, extent, pieces, -0.22, 0.18)
    return jnp.clip(array, -most, most).astype(dtype)


def setup_inputs(seed: int = 0) -> dict:
    streams_of = jax.random.split(jax.random.key(seed), 8)
    return {
        "stiff_bb": centred(streams_of[0], (SETOT, 3, BLK, NB), 1.0, 6.0, ((0, 128),)),
        "stiff_bi": centred(streams_of[1], (SETOT, NB, NI), 1.0, 6.0, ((0, 128),)),
        "constraint_modes": centred(streams_of[2], (SETOT, NI, NB), NI ** -0.5, 0.109375, ((0, 128),)),
        "interior_mass": jnp.clip(jnp.exp(math.log(4.0) - 2.7725887 * jax.random.uniform(streams_of[3], (SETOT, NI), jnp.float32) ** steps_of(streams_of[3], (SETOT, NI), ((0, 128),), -0.2, 0.2)), 0.25, 4.0),
        "fixed_modes": centred(streams_of[4], (SETOT, NI, NM), 1.0, 6.0, ((0, 128),)),
        "mass_bb": centred(streams_of[5], (SETOT, 3, BLK, NB), 1.0, 6.0, ((0, 128),)),
        "boundary_map": draw_boundary_map(jax.random.fold_in(streams_of[7], 71), 0),
    }


PAIRS = ((0, 0), (1, 1), (2, 2), (0, 1), (0, 2), (1, 2))


def reduce_one(items):
    block_bb, block_bi, psi, masses, modes, mass_block = items
    order = block_bi.shape[0]
    weighted = (masses[:, None] * psi.astype(jnp.float32)).astype(jnp.bfloat16)
    red_k = block_bb.reshape(order, order).astype(jnp.float32) + jnp.dot(block_bi, psi, preferred_element_type=jnp.float32)
    red_m = mass_block.reshape(order, order).astype(jnp.float32) + jnp.dot(psi.T, weighted, preferred_element_type=jnp.float32)
    coupling = jnp.dot(modes.T, weighted, preferred_element_type=jnp.float32)
    return red_k, red_m, coupling


def reference(stiff_bb, stiff_bi, constraint_modes, interior_mass, fixed_modes, mass_bb, boundary_map):
    red_k, red_m, coupling = lax.map(reduce_one, (stiff_bb, stiff_bi, constraint_modes, interior_mass, fixed_modes, mass_bb))
    width = stiff_bb.shape[2]
    total_k = jnp.zeros((NBLOCK, BAND, width, width), jnp.float32)
    total_m = jnp.zeros((NBLOCK, BAND, width, width), jnp.float32)
    for first, second in PAIRS:
        rows = boundary_map[:, first].astype(jnp.int32)
        offset = (boundary_map[:, second] - boundary_map[:, first]).astype(jnp.int32)
        piece_k = red_k[:, first * width:(first + 1) * width, second * width:(second + 1) * width]
        piece_m = red_m[:, first * width:(first + 1) * width, second * width:(second + 1) * width]
        total_k = total_k.at[rows, offset].add(piece_k)
        total_m = total_m.at[rows, offset].add(piece_m)
    return total_k, total_m, coupling
```

```python
import functools

import jax
import jax.numpy as jnp
from jax import lax
from jax.experimental import pallas as pl
from jax.experimental.pallas import tpu as pltpu
from jax.sharding import PartitionSpec as P

BAND = 4
BPO = 24
MESH = pl.DeviceIdType.MESH

PAIRS = ((2, 2), (1, 1), (1, 2), (0, 0), (0, 1), (0, 2))
CHUNKS = ((0, 2, 0, 1), (0, 1, 1, 2), (0, 0, 3, 3), (1, 0, 9, 3), (1, 1, 7, 2), (1, 2, 6, 1))


def ring_place(me, t):
    y, x, k = me // 8, (me // 2) % 4, me % 2
    dx = t % 4
    dy = (t // 4 + t) % 4
    dk = t // 16
    return ((y + dy) % 4) * 8 + ((x + dx) % 4) * 2 + (k + dk) % 2


def reduce_and_send(
    owners, lanes,
    map_ref, mass_ref, sbb_hbm, sbi_hbm, psi_hbm, fix_hbm, mbb_hbm,
    recv_hbm, table_ref, coup_hbm,
    psi, sbi, fix, wgt, sbb, mbb, msq, coup, zmap, zmap_s, rmap, rmap_s, pick,
    r0, r1, r2, r3, r4, r5, z0, z1, z2, z3, z4, z5, s0, s1, s2, s3, s4, s5,
    in_sem, coup_sem, zm_send, zm_recv, zm_loc, rm_send, rm_recv, rm_loc,
    z_send, z_recv, x_send, x_recv, x_own,
):
    reds, zs, slots = (r0, r1, r2, r3, r4, r5), (z0, z1, z2, z3, z4, z5), (s0, s1, s2, s3, s4, s5)
    me, lane = lax.axis_index("row"), lax.axis_index("col")
    count, order = psi.shape[0], psi.shape[2]
    width = order // 3
    part = width // lanes

    loads = {}

    def load(name, src, dst, sem):
        loads[name] = pltpu.make_async_copy(src, dst, in_sem.at[sem])
        loads[name].start()

    for i, b in enumerate((2, 1, 0)):
        cols = pl.ds(b * width, width)
        load(("psi", b), psi_hbm.at[:, :, cols], psi.at[:, :, cols], 2 * i)
        load(("sbi", b), sbi_hbm.at[:, cols, :], sbi.at[:, cols, :], 2 * i + 1)
        if i == 0:
            load("sbb", sbb_hbm, sbb, 6)
    load("mbb", mbb_hbm, mbb, 7)
    load("fix", fix_hbm, fix, 8)

    barrier = pltpu.get_barrier_semaphore()
    for d in range(1, lanes):
        pl.semaphore_signal(barrier, inc=1, device_id=(me, lax.rem(lane + d, lanes)), device_id_type=MESH)

    def greet(t, carry):
        pl.semaphore_signal(barrier, inc=1, device_id=(ring_place(me, t), lane), device_id_type=MESH)
        return carry

    lax.fori_loop(1, owners, greet, 0)
    pl.semaphore_wait(barrier, owners + lanes - 2)

    zmap[pl.ds(lane, 1)] = map_ref[...]
    map_sends = []
    for d in range(1, lanes):
        peer = lax.rem(lane + d, lanes)
        copy = pltpu.make_async_remote_copy(
            src_ref=map_ref, dst_ref=zmap.at[pl.ds(lane, 1)], send_sem=zm_send.at[d - 1],
            recv_sem=zm_recv.at[d - 1], device_id=(me, peer), device_id_type=MESH)
        copy.start()
        map_sends.append(copy)

    def stiff_block(b, red):
        n = 3 - b

        def one(s, carry):
            out = jnp.dot(sbi[s, pl.ds(b * width, width), :], psi[s, :, pl.ds(b * width, n * width)],
                          preferred_element_type=jnp.float32)
            out = out + sbb[s, b, :, pl.ds(b * width, n * width)].astype(jnp.float32)
            for q in range(n):
                red[s, q] = out[:, q * width:(q + 1) * width]
            return carry

        lax.fori_loop(0, count, one, 0)

    def mass_block(b, red):
        n = 3 - b

        def one(s, carry):
            out = lax.dot_general(psi[s, :, pl.ds(b * width, width)], wgt[s, :, pl.ds(b * width, n * width)],
                                  (((0,), (0,)), ((), ())), preferred_element_type=jnp.float32)
            out = out + mbb[s, b, :, pl.ds(b * width, n * width)].astype(jnp.float32)
            for q in range(n):
                red[s, q] = out[:, q * width:(q + 1) * width]
            return carry

        lax.fori_loop(0, count, one, 0)

    z_copies = {}

    def send_lanes(c):
        red, z = reds[c], zs[c]
        z[pl.ds(count * lane, count)] = red[:, :, pl.ds(pl.multiple_of(part * lane, part), part), :]
        for d in range(1, lanes):
            peer = lax.rem(lane + d, lanes)
            copy = pltpu.make_async_remote_copy(
                src_ref=red.at[:, :, pl.ds(pl.multiple_of(part * peer, part), part), :],
                dst_ref=z.at[pl.ds(count * lane, count)], send_sem=z_send.at[c, d - 1],
                recv_sem=z_recv.at[c, d - 1], device_id=(me, peer), device_id_type=MESH)
            copy.start()
            z_copies[c, d] = copy

    def send_owners(c):
        z, slot = zs[c], slots[c]
        first, n = CHUNKS[c][2], CHUNKS[c][3]
        for d in range(1, lanes):
            z_copies[c, d].wait_recv()

        def one(t, carry):
            to = ring_place(me, t)
            slot[t] = z[pick[to]]
            pltpu.make_async_remote_copy(
                src_ref=slot.at[t], dst_ref=recv_hbm.at[me, pl.ds(first, n)], send_sem=x_send.at[c],
                recv_sem=x_recv.at[c], device_id=(to, lane), device_id_type=MESH).start()
            return carry

        lax.fori_loop(1, owners, one, 0)
        slot[0] = z[pick[me]]
        pltpu.make_async_copy(slot.at[0], recv_hbm.at[me, pl.ds(first, n)], x_own.at[c]).start()

    loads["psi", 2].wait()
    loads["sbi", 2].wait()
    loads["sbb"].wait()
    stiff_block(2, reds[0])
    send_lanes(0)
    loads["psi", 1].wait()
    loads["sbi", 1].wait()
    stiff_block(1, reds[1])
    send_lanes(1)

    for d in range(1, lanes):
        map_sends[d - 1].wait_recv()
    to_scalars = pltpu.make_async_copy(zmap, zmap_s, zm_loc)
    to_scalars.start()

    def tell(t, carry):
        pltpu.make_async_remote_copy(
            src_ref=zmap, dst_ref=rmap.at[me], send_sem=rm_send, recv_sem=rm_recv,
            device_id=(ring_place(me, t), lane), device_id_type=MESH).start()
        return carry

    lax.fori_loop(1, owners, tell, 0)
    rmap[me] = zmap[...]
    to_scalars.wait()
    heads = [zmap_s[j // count, 0, 3 * (j % count)] // BPO for j in range(lanes * count)]

    def choose(o, carry):
        found = jnp.int32(0)
        for j, head in enumerate(heads):
            found = jnp.where(head == o, jnp.int32(j), found)
        pick[o] = found
        return carry

    lax.fori_loop(0, owners, choose, 0)

    loads["psi", 0].wait()
    loads["sbi", 0].wait()
    stiff_block(0, reds[2])
    send_lanes(2)
    send_owners(0)

    blocks = psi.shape[1] // 128

    def weigh(s, carry):
        turned = msq[s].T
        for a in range(blocks):
            rows = slice(a * 128, (a + 1) * 128)
            wgt[s, rows, :] = (turned[:, a:a + 1] * psi[s, rows, :].astype(jnp.float32)).astype(jnp.bfloat16)
        return carry

    msq[...] = jnp.zeros_like(msq)
    for s in range(count):
        for a in range(blocks):
            msq[s, a:a + 1, :] = mass_ref[s:s + 1, a * 128:(a + 1) * 128]
    lax.fori_loop(0, count, weigh, 0)
    send_owners(1)

    loads["mbb"].wait()
    mass_block(0, reds[3])
    send_lanes(3)
    send_owners(2)
    mass_block(1, reds[4])
    send_lanes(4)
    mass_block(2, reds[5])
    send_lanes(5)
    send_owners(3)

    pltpu.make_async_copy(rmap.at[pl.ds(0, owners - 1)], rmap.at[pl.ds(0, owners - 1)], rm_recv).wait()
    to_scalars = pltpu.make_async_copy(rmap, rmap_s, rm_loc)
    to_scalars.start()
    to_scalars.wait()

    def place(r, carry):
        found = [jnp.int32(-1)] * 3
        for j in range(lanes * count):
            got = [rmap_s[r, j // count, 0, 3 * (j % count) + i] for i in range(3)]
            mine = got[0] // BPO == me
            found = [jnp.where(mine, g - me * BPO, f) for g, f in zip(got, found)]
        for i in range(3):
            table_ref[r, i] = found[i]
        return carry

    lax.fori_loop(0, owners, place, 0)

    loads["fix"].wait()

    def couple(s, carry):
        coup[s] = lax.dot_general(fix[s], wgt[s], (((0,), (0,)), ((), ())), preferred_element_type=jnp.float32)
        return carry

    lax.fori_loop(0, count, couple, 0)
    coup_copy = pltpu.make_async_copy(coup, coup_hbm, coup_sem)
    coup_copy.start()
    send_owners(4)
    send_owners(5)

    coup_copy.wait()
    for d in range(1, lanes):
        map_sends[d - 1].wait_send()
    pltpu.make_async_copy(rmap.at[pl.ds(0, owners - 1)], rmap.at[pl.ds(0, owners - 1)], rm_send).wait()
    for c, (_, _, first, n) in enumerate(CHUNKS):
        for d in range(1, lanes):
            z_copies[c, d].wait_send()
        pltpu.make_async_copy(slots[c].at[0], recv_hbm.at[me, pl.ds(first, n)], x_own.at[c]).wait()
        sent = slots[c].at[pl.ds(1, owners - 1)]
        pltpu.make_async_copy(sent, sent, x_send.at[c]).wait()
        pltpu.make_async_copy(sent, sent, x_recv.at[c]).wait()


def assemble(owners, table_ref, recv_hbm, k_ref, m_ref, buf, sem):
    def fetch(r):
        return pltpu.make_async_copy(recv_hbm.at[r], buf.at[r], sem.at[r])

    def begin(r, carry):
        @pl.when(table_ref[r, 0] >= 0)
        def _():
            fetch(r).start()

        return carry

    lax.fori_loop(0, owners, begin, 0)

    def clear(e, carry):
        k_ref[e] = jnp.zeros(k_ref.shape[1:], jnp.float32)
        m_ref[e] = jnp.zeros(m_ref.shape[1:], jnp.float32)
        return carry

    lax.fori_loop(0, BPO * BAND, clear, 0)

    def add(r, carry):
        @pl.when(table_ref[r, 0] >= 0)
        def _():
            places = [table_ref[r, i] for i in range(3)]
            fetch(r).wait()
            for p, (i, j) in enumerate(PAIRS):
                e = places[i] * BAND + places[j] - places[i]
                k_ref[e] += buf[r, p]
                m_ref[e] += buf[r, len(PAIRS) + p]

        return carry

    lax.fori_loop(0, owners, add, 0)


def per_device(stiff_bb, stiff_bi, constraint_modes, interior_mass, fixed_modes, mass_bb, boundary_map):
    owners, lanes = lax.axis_size("row"), lax.axis_size("col")
    count, inner, order = constraint_modes.shape
    modes = fixed_modes.shape[2]
    width = order // 3
    part = width // lanes
    planes = 2 * len(PAIRS)
    maps = jnp.pad(boundary_map.reshape(1, 1, 3 * count), ((0, 0), (0, 0), (0, 128 - 3 * count)))

    anywhere = pl.BlockSpec(memory_space=pl.ANY)
    in_vmem = pl.BlockSpec(memory_space=pltpu.VMEM)
    f32, bf16, i32 = jnp.float32, jnp.bfloat16, jnp.int32
    dma = pltpu.SemaphoreType.DMA
    received, table, coupling = pl.pallas_call(
        functools.partial(reduce_and_send, owners, lanes),
        out_shape=(
            jax.ShapeDtypeStruct((owners, planes, part, width), f32),
            jax.ShapeDtypeStruct((owners, 4), i32),
            jax.ShapeDtypeStruct((count, modes, order), f32),
        ),
        in_specs=[in_vmem, in_vmem] + [anywhere] * 5,
        out_specs=(anywhere, pl.BlockSpec(memory_space=pltpu.SMEM), anywhere),
        scratch_shapes=[
            pltpu.VMEM((count, inner, order), bf16),
            pltpu.VMEM((count, order, inner), bf16),
            pltpu.VMEM((count, inner, modes), bf16),
            pltpu.VMEM((count, inner, order), bf16),
            pltpu.VMEM((count, 3, width, order), bf16),
            pltpu.VMEM((count, 3, width, order), bf16),
            pltpu.VMEM((count, 128, 128), f32),
            pltpu.VMEM((count, modes, order), f32),
            pltpu.VMEM((lanes, 1, 128), i32),
            pltpu.SMEM((lanes, 1, 128), i32),
            pltpu.VMEM((owners, lanes, 1, 128), i32),
            pltpu.SMEM((owners, lanes, 1, 128), i32),
            pltpu.SMEM((owners,), i32),
        ]
        + [pltpu.VMEM((count, n, width, width), f32) for _, _, _, n in CHUNKS]
        + [pltpu.VMEM((count * lanes, n, part, width), f32) for _, _, _, n in CHUNKS]
        + [pltpu.VMEM((owners, n, part, width), f32) for _, _, _, n in CHUNKS]
        + [
            dma((9,)), dma, dma((lanes - 1,)), dma((lanes - 1,)), dma, dma, dma, dma,
            dma((len(CHUNKS), lanes - 1)), dma((len(CHUNKS), lanes - 1)),
            dma((len(CHUNKS),)), dma((len(CHUNKS),)), dma((len(CHUNKS),)),
        ],
        compiler_params=pltpu.CompilerParams(
            collective_id=0, has_side_effects=True, vmem_limit_bytes=60 * 1024 * 1024),
        name="reduce_and_send",
    )(maps, interior_mass, stiff_bb, stiff_bi, constraint_modes, fixed_modes, mass_bb)

    entry = jax.ShapeDtypeStruct((BPO * BAND, part, width), f32)
    k_band, m_band = pl.pallas_call(
        functools.partial(assemble, owners),
        out_shape=(entry, entry),
        in_specs=[pl.BlockSpec(memory_space=pltpu.SMEM), anywhere],
        out_specs=(in_vmem, in_vmem),
        scratch_shapes=[pltpu.VMEM((owners, planes, part, width), f32), dma((owners,))],
        compiler_params=pltpu.CompilerParams(vmem_limit_bytes=40 * 1024 * 1024),
        name="assemble",
    )(table, received)
    banded = (BPO, BAND, part, width)
    return k_band.reshape(banded), m_band.reshape(banded), coupling


def solution(mesh):
    both = ("row", "col")
    return jax.shard_map(
        per_device,
        mesh=mesh,
        in_specs=(
            P(both, None, None, None), P(both, None, None), P(both, None, None), P(both, None),
            P(both, None, None), P(both, None, None, None), P(both, None),
        ),
        out_specs=(P("row", None, "col", None), P("row", None, "col", None), P(both, None, None)),
        check_vma=False,
    )
```

```python
import functools

import jax
import jax.numpy as jnp
from jax import lax
from jax.experimental import pallas as pl
from jax.experimental.pallas import tpu as pltpu
from jax.sharding import PartitionSpec as P

BAND = 4
BPO = 24
MESH = pl.DeviceIdType.MESH

PAIRS = ((2, 2), (1, 1), (1, 2), (0, 0), (0, 1), (0, 2))
CHUNKS = ((0, 2, 0, 1), (0, 1, 1, 2), (0, 0, 3, 3), (1, 0, 9, 3), (1, 1, 7, 2), (1, 2, 6, 1))


def ring_place(me, t):
    y, x, k = me // 8, (me // 2) % 4, me % 2
    dx = t % 4
    dy = (t // 4 + t) % 4
    dk = t // 16
    return ((y + dy) % 4) * 8 + ((x + dx) % 4) * 2 + (k + dk) % 2


def reduce_and_send(
    owners, lanes,
    map_hbm, mass_hbm, sbb_hbm, sbi_hbm, psi_hbm, fix_hbm, mbb_hbm,
    recv_hbm, table_hbm, coup_hbm,
    psi, sbi, fix, wgt, sbb, mbb, mass, msq, coup, map_s, mine, zmap, zmap_s, rmap, rmap_s, pick, table,
    r0, r1, r2, r3, r4, r5, z0, z1, z2, z3, z4, z5, s0, s1, s2, s3, s4, s5,
    in_sem, coup_sem, table_sem, zm_send, zm_recv, zm_loc, rm_send, rm_recv, rm_loc,
    z_send, z_recv, x_send, x_recv, x_own,
):
    reds, zs, slots = (r0, r1, r2, r3, r4, r5), (z0, z1, z2, z3, z4, z5), (s0, s1, s2, s3, s4, s5)
    me, lane = lax.axis_index("row"), lax.axis_index("col")
    count, order = psi.shape[0], psi.shape[2]
    width = order // 3
    part = width // lanes

    loads = {}

    def load(name, src, dst):
        loads[name] = pltpu.make_async_copy(src, dst, in_sem.at[len(loads)])
        loads[name].start()

    def load_block(b):
        cols = pl.ds(b * width, width)
        load(("psi", b), psi_hbm.at[:, :, cols], psi.at[:, :, cols])
        load(("sbi", b), sbi_hbm.at[:, cols, :], sbi.at[:, cols, :])
        load(("sbb", b), sbb_hbm.at[:, b], sbb.at[:, b])

    def loaded(b):
        for name in ("psi", "sbi", "sbb"):
            loads[name, b].wait()

    load("map", map_hbm, map_s)
    load_block(2)

    barrier = pltpu.get_barrier_semaphore()
    for d in range(1, lanes):
        pl.semaphore_signal(barrier, inc=1, device_id=(me, lax.rem(lane + d, lanes)), device_id_type=MESH)

    def greet(t, carry):
        pl.semaphore_signal(barrier, inc=1, device_id=(ring_place(me, t), lane), device_id_type=MESH)
        return carry

    loads["map"].wait()
    lanes_of = lax.broadcasted_iota(jnp.int32, (1, 1, 128), 2)

    def as_row(scalars):
        row = jnp.zeros((1, 1, 128), jnp.int32)
        for i, scalar in enumerate(scalars):
            row = jnp.where(lanes_of == i, scalar, row)
        return row

    own = as_row([map_s[s, i] for s in range(count) for i in range(3)])
    mine[...] = own
    zmap[pl.ds(lane, 1)] = own
    lax.fori_loop(1, owners, greet, 0)
    pl.semaphore_wait(barrier, owners + lanes - 2)
    map_sends = []
    for d in range(1, lanes):
        peer = lax.rem(lane + d, lanes)
        copy = pltpu.make_async_remote_copy(
            src_ref=mine, dst_ref=zmap.at[pl.ds(lane, 1)], send_sem=zm_send.at[d - 1],
            recv_sem=zm_recv.at[d - 1], device_id=(me, peer), device_id_type=MESH)
        copy.start()
        map_sends.append(copy)

    def stiff_block(b, red):
        n = 3 - b

        def one(s, carry):
            out = jnp.dot(sbi[s, pl.ds(b * width, width), :], psi[s, :, pl.ds(b * width, n * width)],
                          preferred_element_type=jnp.float32)
            out = out + sbb[s, b, :, pl.ds(b * width, n * width)].astype(jnp.float32)
            for q in range(n):
                red[s, q] = out[:, q * width:(q + 1) * width]
            return carry

        lax.fori_loop(0, count, one, 0)

    def mass_block(b, red):
        n = 3 - b

        def one(s, carry):
            out = lax.dot_general(psi[s, :, pl.ds(b * width, width)], wgt[s, :, pl.ds(b * width, n * width)],
                                  (((0,), (0,)), ((), ())), preferred_element_type=jnp.float32)
            out = out + mbb[s, b, :, pl.ds(b * width, n * width)].astype(jnp.float32)
            for q in range(n):
                red[s, q] = out[:, q * width:(q + 1) * width]
            return carry

        lax.fori_loop(0, count, one, 0)

    z_copies = {}

    def send_lanes(c):
        red, z = reds[c], zs[c]
        z[pl.ds(count * lane, count)] = red[:, :, pl.ds(pl.multiple_of(part * lane, part), part), :]
        for d in range(1, lanes):
            peer = lax.rem(lane + d, lanes)
            copy = pltpu.make_async_remote_copy(
                src_ref=red.at[:, :, pl.ds(pl.multiple_of(part * peer, part), part), :],
                dst_ref=z.at[pl.ds(count * lane, count)], send_sem=z_send.at[c, d - 1],
                recv_sem=z_recv.at[c, d - 1], device_id=(me, peer), device_id_type=MESH)
            copy.start()
            z_copies[c, d] = copy

    def send_owners(c):
        z, slot = zs[c], slots[c]
        first, n = CHUNKS[c][2], CHUNKS[c][3]
        for d in range(1, lanes):
            z_copies[c, d].wait_recv()

        def one(t, carry):
            to = ring_place(me, t)
            slot[t] = z[pick[to]]
            pltpu.make_async_remote_copy(
                src_ref=slot.at[t], dst_ref=recv_hbm.at[me, pl.ds(first, n)], send_sem=x_send.at[c],
                recv_sem=x_recv.at[c], device_id=(to, lane), device_id_type=MESH).start()
            return carry

        lax.fori_loop(1, owners, one, 0)
        slot[0] = z[pick[me]]
        pltpu.make_async_copy(slot.at[0], recv_hbm.at[me, pl.ds(first, n)], x_own.at[c]).start()

    loaded(2)
    load_block(1)
    stiff_block(2, reds[0])
    send_lanes(0)
    loaded(1)
    load_block(0)
    stiff_block(1, reds[1])
    send_lanes(1)

    for d in range(1, lanes):
        map_sends[d - 1].wait_recv()
    to_scalars = pltpu.make_async_copy(zmap, zmap_s, zm_loc)
    to_scalars.start()

    def tell(t, carry):
        pltpu.make_async_remote_copy(
            src_ref=zmap, dst_ref=rmap.at[me], send_sem=rm_send, recv_sem=rm_recv,
            device_id=(ring_place(me, t), lane), device_id_type=MESH).start()
        return carry

    lax.fori_loop(1, owners, tell, 0)
    rmap[me] = zmap[...]
    to_scalars.wait()
    heads = [zmap_s[j // count, 0, 3 * (j % count)] // BPO for j in range(lanes * count)]

    def choose(o, carry):
        found = jnp.int32(0)
        for j, head in enumerate(heads):
            found = jnp.where(head == o, jnp.int32(j), found)
        pick[o] = found
        return carry

    lax.fori_loop(0, owners, choose, 0)

    loaded(0)
    load("mass", mass_hbm, mass)
    load("mbb", mbb_hbm, mbb)
    load("fix", fix_hbm, fix)
    stiff_block(0, reds[2])
    send_lanes(2)
    send_owners(0)

    blocks = psi.shape[1] // 128

    def weigh(s, carry):
        turned = msq[s].T
        for a in range(blocks):
            rows = slice(a * 128, (a + 1) * 128)
            wgt[s, rows, :] = (turned[:, a:a + 1] * psi[s, rows, :].astype(jnp.float32)).astype(jnp.bfloat16)
        return carry

    msq[...] = jnp.zeros_like(msq)
    loads["mass"].wait()
    for s in range(count):
        for a in range(blocks):
            msq[s, a:a + 1, :] = mass[s:s + 1, a * 128:(a + 1) * 128]
    lax.fori_loop(0, count, weigh, 0)
    send_owners(1)

    loads["mbb"].wait()
    mass_block(0, reds[3])
    send_lanes(3)
    send_owners(2)
    mass_block(1, reds[4])
    send_lanes(4)
    mass_block(2, reds[5])
    send_lanes(5)
    send_owners(3)

    pltpu.make_async_copy(rmap.at[pl.ds(0, owners - 1)], rmap.at[pl.ds(0, owners - 1)], rm_recv).wait()
    to_scalars = pltpu.make_async_copy(rmap, rmap_s, rm_loc)
    to_scalars.start()
    to_scalars.wait()

    def place(r, carry):
        found = [jnp.int32(-1)] * 3
        for j in range(lanes * count):
            got = [rmap_s[r, j // count, 0, 3 * (j % count) + i] for i in range(3)]
            mine = got[0] // BPO == me
            found = [jnp.where(mine, g - me * BPO, f) for g, f in zip(got, found)]
        table[pl.ds(r, 1)] = as_row(found)
        return carry

    lax.fori_loop(0, owners, place, 0)
    table_copy = pltpu.make_async_copy(table, table_hbm, table_sem)

    loads["fix"].wait()

    def couple(s, carry):
        coup[s] = lax.dot_general(fix[s], wgt[s], (((0,), (0,)), ((), ())), preferred_element_type=jnp.float32)
        return carry

    lax.fori_loop(0, count, couple, 0)
    coup_copy = pltpu.make_async_copy(coup, coup_hbm, coup_sem)
    coup_copy.start()
    table_copy.start()
    send_owners(4)
    send_owners(5)

    coup_copy.wait()
    table_copy.wait()
    for d in range(1, lanes):
        map_sends[d - 1].wait_send()
    pltpu.make_async_copy(rmap.at[pl.ds(0, owners - 1)], rmap.at[pl.ds(0, owners - 1)], rm_send).wait()
    for c, (_, _, first, n) in enumerate(CHUNKS):
        for d in range(1, lanes):
            z_copies[c, d].wait_send()
        pltpu.make_async_copy(slots[c].at[0], recv_hbm.at[me, pl.ds(first, n)], x_own.at[c]).wait()
        sent = slots[c].at[pl.ds(1, owners - 1)]
        pltpu.make_async_copy(sent, sent, x_send.at[c]).wait()
        pltpu.make_async_copy(sent, sent, x_recv.at[c]).wait()


def assemble(
    owners, table_hbm, recv_hbm, coup_hbm, k_hbm, m_hbm, coup_out,
    table, buf, k_acc, m_acc, coup, table_sem, k_sem, m_sem, out_sem, coup_in, coup_back,
):
    half = len(PAIRS)
    to_scalars = pltpu.make_async_copy(table_hbm, table, table_sem)
    to_scalars.start()

    def fetch(r, mat, sem):
        planes = pl.ds(mat * half, half)
        return pltpu.make_async_copy(recv_hbm.at[r, planes], buf.at[r, planes], sem.at[r])

    def begin(mat, sem):
        def one(r, carry):
            fetch(r, mat, sem).start()
            return carry

        lax.fori_loop(0, owners, one, 0)

    begin(0, k_sem)
    begin(1, m_sem)
    take = pltpu.make_async_copy(coup_hbm, coup, coup_in)
    take.start()

    def clear(e, carry):
        k_acc[e] = jnp.zeros(k_acc.shape[1:], jnp.float32)
        m_acc[e] = jnp.zeros(m_acc.shape[1:], jnp.float32)
        return carry

    lax.fori_loop(0, BPO * BAND, clear, 0)
    to_scalars.wait()

    def add(acc, mat, sem):
        def one(r, carry):
            fetch(r, mat, sem).wait()
            places = [table[r, 0, i] for i in range(3)]

            @pl.when(places[0] >= 0)
            def _():
                entries = [places[i] * BAND + places[j] - places[i] for i, j in PAIRS]
                sums = [acc[e] + buf[r, mat * half + p] for p, e in enumerate(entries)]
                for e, total in zip(entries, sums):
                    acc[e] = total

            return carry

        lax.fori_loop(0, owners, one, 0)

    add(k_acc, 0, k_sem)
    k_out = pltpu.make_async_copy(k_acc, k_hbm, out_sem.at[0])
    k_out.start()
    take.wait()
    give = pltpu.make_async_copy(coup, coup_out, coup_back)
    give.start()
    add(m_acc, 1, m_sem)
    m_out = pltpu.make_async_copy(m_acc, m_hbm, out_sem.at[1])
    m_out.start()
    k_out.wait()
    give.wait()
    m_out.wait()


def per_device(stiff_bb, stiff_bi, constraint_modes, interior_mass, fixed_modes, mass_bb, boundary_map):
    owners, lanes = lax.axis_size("row"), lax.axis_size("col")
    count, inner, order = constraint_modes.shape
    modes = fixed_modes.shape[2]
    width = order // 3
    part = width // lanes
    planes = 2 * len(PAIRS)

    anywhere = pl.BlockSpec(memory_space=pl.ANY)
    f32, bf16, i32 = jnp.float32, jnp.bfloat16, jnp.int32
    dma = pltpu.SemaphoreType.DMA
    received, table, coupling = pl.pallas_call(
        functools.partial(reduce_and_send, owners, lanes),
        out_shape=(
            jax.ShapeDtypeStruct((owners, planes, part, width), f32),
            jax.ShapeDtypeStruct((owners, 1, 128), i32),
            jax.ShapeDtypeStruct((count, modes, order), f32),
        ),
        in_specs=[anywhere] * 7,
        out_specs=(anywhere, anywhere, anywhere),
        scratch_shapes=[
            pltpu.VMEM((count, inner, order), bf16),
            pltpu.VMEM((count, order, inner), bf16),
            pltpu.VMEM((count, inner, modes), bf16),
            pltpu.VMEM((count, inner, order), bf16),
            pltpu.VMEM((count, 3, width, order), bf16),
            pltpu.VMEM((count, 3, width, order), bf16),
            pltpu.VMEM((count, inner), f32),
            pltpu.VMEM((count, 128, 128), f32),
            pltpu.VMEM((count, modes, order), f32),
            pltpu.SMEM((count, 3), i32),
            pltpu.VMEM((1, 1, 128), i32),
            pltpu.VMEM((lanes, 1, 128), i32),
            pltpu.SMEM((lanes, 1, 128), i32),
            pltpu.VMEM((owners, lanes, 1, 128), i32),
            pltpu.SMEM((owners, lanes, 1, 128), i32),
            pltpu.SMEM((owners,), i32),
            pltpu.VMEM((owners, 1, 128), i32),
        ]
        + [pltpu.VMEM((count, n, width, width), f32) for _, _, _, n in CHUNKS]
        + [pltpu.VMEM((count * lanes, n, part, width), f32) for _, _, _, n in CHUNKS]
        + [pltpu.VMEM((owners, n, part, width), f32) for _, _, _, n in CHUNKS]
        + [
            dma((13,)), dma, dma, dma((lanes - 1,)), dma((lanes - 1,)), dma, dma, dma, dma,
            dma((len(CHUNKS), lanes - 1)), dma((len(CHUNKS), lanes - 1)),
            dma((len(CHUNKS),)), dma((len(CHUNKS),)), dma((len(CHUNKS),)),
        ],
        compiler_params=pltpu.CompilerParams(
            collective_id=0, has_side_effects=True, vmem_limit_bytes=60 * 1024 * 1024),
        name="reduce_and_send",
    )(boundary_map, interior_mass, stiff_bb, stiff_bi, constraint_modes, fixed_modes, mass_bb)

    entry = (BPO * BAND, part, width)
    in_hbm = pl.BlockSpec(memory_space=pltpu.HBM)
    k_band, m_band, coupling = pl.pallas_call(
        functools.partial(assemble, owners),
        out_shape=(
            jax.ShapeDtypeStruct(entry, f32),
            jax.ShapeDtypeStruct(entry, f32),
            jax.ShapeDtypeStruct((count, modes, order), f32),
        ),
        in_specs=[in_hbm] * 3,
        out_specs=[in_hbm] * 3,
        scratch_shapes=[
            pltpu.SMEM((owners, 1, 128), i32),
            pltpu.VMEM((owners, planes, part, width), f32),
            pltpu.VMEM(entry, f32),
            pltpu.VMEM(entry, f32),
            pltpu.VMEM((count, modes, order), f32),
            dma, dma((owners,)), dma((owners,)), dma((2,)), dma, dma,
        ],
        compiler_params=pltpu.CompilerParams(vmem_limit_bytes=60 * 1024 * 1024),
        name="assemble",
    )(table, received, coupling)
    banded = (BPO, BAND, part, width)
    return k_band.reshape(banded), m_band.reshape(banded), coupling


def solution(mesh):
    both = ("row", "col")
    return jax.shard_map(
        per_device,
        mesh=mesh,
        in_specs=(
            P(both, None, None, None), P(both, None, None), P(both, None, None), P(both, None),
            P(both, None, None), P(both, None, None, None), P(both, None),
        ),
        out_specs=(P("row", None, "col", None), P("row", None, "col", None), P(both, None, None)),
        check_vma=False,
    )
```

```python
import functools

import jax
import jax.numpy as jnp
from jax import lax
from jax.experimental import pallas as pl
from jax.experimental.pallas import tpu as pltpu
from jax.sharding import PartitionSpec as P

BAND = 4
LAGS = (1, 3)
BPO = 24
MESH = pl.DeviceIdType.MESH

PAIRS = ((2, 2), (1, 1), (1, 2), (0, 0), (0, 1), (0, 2))
BLOCKS = ((0, 2), (0, 1), (0, 0), (1, 0), (1, 1), (1, 2))
CHUNKS = tuple(
    (i, q, mat * len(PAIRS) + (0, 1, 3)[2 - b] + q) for i, (mat, b) in enumerate(BLOCKS) for q in range(3 - b)
)


def row_of(y, x, k):
    return y * 8 + x * 2 + k


def place(h, f, g, k):
    return row_of(f, g, k) if h == 0 else row_of(g, f, k)


def owner_of(block):
    return lax.shift_right_logical(block * 2731, jnp.int32(16))


def first_axis(h, owner):
    return lax.shift_right_logical(owner, jnp.int32(3)) if h == 0 else lax.shift_right_logical(owner, jnp.int32(1)) & 3


def count_before(flags):
    total, before = jnp.int32(0), []
    for flag in flags:
        before.append(total)
        total = total + jnp.where(flag, 1, 0)
    return before, total


def find(keys, values, wanted):
    found = jnp.int32(0)
    for key, value in zip(keys, values):
        found = jnp.where(key == wanted, value, found)
    return found


def reduce_and_send(
    owners, lanes,
    map_hbm, mass_hbm, sbb_hbm, sbi_hbm, psi_hbm, fix_hbm, mbb_hbm,
    recv0_hbm, recv1_hbm, table_hbm, coup_hbm,
    psi, sbi, fix, wgt, sbb, mbb, mass, msq, coup, map_s, mine, zmap, whole, whole_s, rmap, rmap_s, pick1, pick2, table,
    *rest,
):
    n_chunks = len(CHUNKS)
    reds, rest = rest[:len(BLOCKS)], rest[len(BLOCKS):]
    zs, firsts, arrived, seconds = (rest[i * n_chunks:(i + 1) * n_chunks] for i in range(4))
    (in_sem, coup_sem, table_sem, zm_send, zm_recv, zm_loc, rm_send, rm_recv, rm_loc,
     z_send, z_recv, f_send, f_recv, p_send, p_recv, x_send, x_recv, x_own) = rest[4 * n_chunks:]
    recvs = (recv0_hbm, recv1_hbm)
    me, lane = lax.axis_index("row"), lax.axis_index("col")
    y, x, core = me // 8, (me // 2) % 4, me % 2
    at = [(y, x), (x, y)]
    beside = [[place(h, (f + step) % 4, g, core) for step in (1, 3)] for h, (f, g) in enumerate(at)]
    line = [[place(h, f, (g + t // 2) % 4, (core + t) % 2) for t in range(8)] for h, (f, g) in enumerate(at)]
    from_here = [pl.ds((g * 2 + core) * 4, 4) for _, g in at]
    count, order = psi.shape[0], psi.shape[2]
    width = order // 3
    part = width // lanes
    half = part // 2
    group = lanes * count

    loads = {}

    def load(name, src, dst):
        loads[name] = pltpu.make_async_copy(src, dst, in_sem.at[len(loads)])
        loads[name].start()

    def load_block(b):
        cols = pl.ds(b * width, width)
        load(("psi", b), psi_hbm.at[:, :, cols], psi.at[:, :, cols])
        load(("sbi", b), sbi_hbm.at[:, cols, :], sbi.at[:, cols, :])
        load(("sbb", b), sbb_hbm.at[:, b], sbb.at[:, b])

    def loaded(b):
        for name in ("psi", "sbi", "sbb"):
            loads[name, b].wait()

    load("map", map_hbm, map_s)
    load_block(2)

    barrier = pltpu.get_barrier_semaphore()
    for d in range(1, lanes):
        pl.semaphore_signal(barrier, inc=1, device_id=(me, lax.rem(lane + d, lanes)), device_id_type=MESH)

    def greet(t, carry):
        pl.semaphore_signal(barrier, inc=1, device_id=(lax.rem(me + t, owners), lane), device_id_type=MESH)
        return carry

    lax.fori_loop(1, owners, greet, 0)

    loads["map"].wait()
    lanes_of = lax.broadcasted_iota(jnp.int32, (1, 1, 128), 2)

    def as_row(scalars, offset):
        row = jnp.zeros((1, 1, 128), jnp.int32)
        for i, scalar in enumerate(scalars):
            row = jnp.where(lanes_of == offset + i, scalar, row)
        return row

    own = as_row([map_s[s, i] for s in range(count) for i in range(3)], 3 * count * lane)
    mine[...] = own
    zmap[pl.ds(lane, 1)] = own
    pl.semaphore_wait(barrier, owners + lanes - 2)
    map_sends = []
    for d in range(1, lanes):
        peer = lax.rem(lane + d, lanes)
        copy = pltpu.make_async_remote_copy(
            src_ref=mine, dst_ref=zmap.at[pl.ds(lane, 1)], send_sem=zm_send.at[d - 1],
            recv_sem=zm_recv.at[d - 1], device_id=(me, peer), device_id_type=MESH)
        copy.start()
        map_sends.append(copy)

    def stiff_block(b, red):
        n = 3 - b

        def one(s, carry):
            out = jnp.dot(sbi[s, pl.ds(b * width, width), :], psi[s, :, pl.ds(b * width, n * width)],
                          preferred_element_type=jnp.float32)
            out = out + sbb[s, b, :, pl.ds(b * width, n * width)].astype(jnp.float32)
            for q in range(n):
                red[s, q] = out[:, q * width:(q + 1) * width]
            return carry

        lax.fori_loop(0, count, one, 0)

    def mass_block(b, red):
        n = 3 - b

        def one(s, carry):
            out = lax.dot_general(psi[s, :, pl.ds(b * width, width)], wgt[s, :, pl.ds(b * width, n * width)],
                                  (((0,), (0,)), ((), ())), preferred_element_type=jnp.float32)
            out = out + mbb[s, b, :, pl.ds(b * width, n * width)].astype(jnp.float32)
            for q in range(n):
                red[s, q] = out[:, q * width:(q + 1) * width]
            return carry

        lax.fori_loop(0, count, one, 0)

    z_copies, f_copies, p_copies = {}, {}, {}

    def send_lanes(c):
        red, q, z = reds[CHUNKS[c][0]], CHUNKS[c][1], zs[c]
        ours = pl.ds(count * lane, count)
        for h in range(2):
            z[ours, h] = red[:, q, pl.ds(pl.multiple_of(part * lane + half * h, half), half), :]
        for d in range(1, lanes):
            peer = lax.rem(lane + d, lanes)
            for h in range(2):
                copy = pltpu.make_async_remote_copy(
                    src_ref=red.at[:, q, pl.ds(pl.multiple_of(part * peer + half * h, half), half), :],
                    dst_ref=z.at[ours, h], send_sem=z_send.at[c, h, d - 1],
                    recv_sem=z_recv.at[c, h, d - 1], device_id=(me, peer), device_id_type=MESH)
                copy.start()
                z_copies[c, h, d] = copy

    def first_leg(c):
        z, first = zs[c], firsts[c]
        for copy in [z_copies[c, h, d] for h in range(2) for d in range(1, lanes)]:
            copy.wait_recv()
        for h in range(2):
            slots = [z[pick1[h * 16 + t], h] for t in range(16)]
            for t in range(16):
                first[h, t] = slots[t]
        for h in range(2):
            for way in range(2):
                copy = pltpu.make_async_remote_copy(
                    src_ref=first.at[h, pl.ds(8 * way, 8)], dst_ref=arrived[c].at[h, pl.ds(8 * way, 8)],
                    send_sem=f_send.at[c, h, way], recv_sem=f_recv.at[c, h, way],
                    device_id=(beside[h][way], lane), device_id_type=MESH)
                copy.start()
                f_copies[c, h, way] = copy

    def pass_on(c):
        for h in range(2):
            for way in range(2):
                f_copies[c, h, way].wait_recv()
                copy = pltpu.make_async_remote_copy(
                    src_ref=arrived[c].at[h, pl.ds(8 * way + 4, 4)], dst_ref=arrived[c].at[h, pl.ds(16 + 4 * way, 4)],
                    send_sem=p_send.at[c, h, way], recv_sem=p_recv.at[c, h, way],
                    device_id=(beside[h][way], lane), device_id_type=MESH)
                copy.start()
                p_copies[c, h, way] = copy

    def own_copy(c, h):
        return pltpu.make_async_copy(
            seconds[c].at[h, pl.ds(0, 4)], recvs[h].at[from_here[h], CHUNKS[c][2]], x_own.at[c, h])

    def second_leg(c):
        z, second = zs[c], seconds[c]
        for copy in [p_copies[c, h, way] for h in range(2) for way in range(2)]:
            copy.wait_recv()
        for h in range(2):
            for low in (0, 16):
                picked = [
                    z[pick2[h * 32 + i], h] if i % 4 == 0 else arrived[c][h, pick2[h * 32 + i]]
                    for i in range(low, low + 16)
                ]
                for i, value in enumerate(picked):
                    second[h, low + i] = value
            own_copy(c, h).start()
        for t in range(1, 8):
            for h in range(2):
                pltpu.make_async_remote_copy(
                    src_ref=second.at[h, pl.ds(t * 4, 4)], dst_ref=recvs[h].at[from_here[h], CHUNKS[c][2]],
                    send_sem=x_send.at[c, h], recv_sem=x_recv.at[c, h],
                    device_id=(line[h][t], lane), device_id_type=MESH).start()

    def first_tables():
        heads = [owner_of(whole_s[0, 0, 3 * j]) for j in range(group)]
        numbers = [jnp.int32(j) for j in range(group)]
        for h in range(2):
            f = at[h][0]
            away = [(first_axis(h, head) + 4 - f) & 3 for head in heads]
            near, n1 = count_before([a == 1 for a in away])
            far, n2 = count_before([a == 2 for a in away])
            back, _ = count_before([a == 3 for a in away])
            split = jnp.minimum(jnp.minimum(n2, 8 - n1), 4)
            plus = [jnp.where(a == 1, r1, jnp.where((a == 2) & (r2 < split), 7 - r2, -1))
                    for a, r1, r2 in zip(away, near, far)]
            minus = [jnp.where(a == 3, r3, jnp.where((a == 2) & (r2 >= split), 7 + split - r2, -1))
                     for a, r3, r2 in zip(away, back, far)]
            for t in range(8):
                pick1[h * 16 + t] = find(plus, numbers, t)
                pick1[h * 16 + 8 + t] = find(minus, numbers, t)
            for t in range(8):
                pick2[h * 32 + t * 4] = find(heads, numbers, line[h][t])

    def second_tables():
        for h in range(2):
            f, g = at[h]
            for d in range(1, 4):
                source = place(h, (f + 4 - d) % 4, g, core)
                heads = [owner_of(rmap_s[source, 0, 3 * j]) for j in range(group)]
                axis = [first_axis(h, head) for head in heads]
                rank, n2 = count_before([a == f for a in axis])
                if d == 1:
                    spot = rank
                elif d == 3:
                    spot = [8 + r for r in rank]
                else:
                    _, n1 = count_before([a == (f + 3) % 4 for a in axis])
                    split = jnp.minimum(jnp.minimum(n2, 8 - n1), 4)
                    spot = [jnp.where(r < split, 19 - r, 23 + split - r) for r in rank]
                for t in range(8):
                    pick2[h * 32 + t * 4 + d] = find(heads, spot, line[h][t])

    def step(c):
        if c < n_chunks:
            first_leg(c)
        if 0 <= c - LAGS[0] < n_chunks:
            pass_on(c - LAGS[0])
        if 0 <= c - LAGS[1] < n_chunks:
            second_leg(c - LAGS[1])

    loaded(2)
    load_block(1)
    stiff_block(2, reds[0])
    send_lanes(0)
    loaded(1)
    load_block(0)
    stiff_block(1, reds[1])
    send_lanes(1)
    send_lanes(2)

    for d in range(1, lanes):
        map_sends[d - 1].wait_recv()
    merged = zmap[0:1]
    for i in range(1, lanes):
        merged = merged + zmap[i:i + 1]
    whole[...] = merged
    rmap[pl.ds(me, 1)] = merged
    to_scalars = pltpu.make_async_copy(whole, whole_s, zm_loc)
    to_scalars.start()

    to_scalars.wait()
    first_tables()
    step(0)

    def tell(t, carry):
        pltpu.make_async_remote_copy(
            src_ref=whole, dst_ref=rmap.at[pl.ds(me, 1)], send_sem=rm_send, recv_sem=rm_recv,
            device_id=(lax.rem(me + t, owners), lane), device_id_type=MESH).start()
        return carry

    lax.fori_loop(1, owners, tell, 0)
    loaded(0)
    load("mass", mass_hbm, mass)
    load("mbb", mbb_hbm, mbb)
    load("fix", fix_hbm, fix)
    stiff_block(0, reds[2])
    for c in (3, 4, 5):
        send_lanes(c)
    step(1)

    others = rmap.at[pl.ds(0, owners - 1)]
    pltpu.make_async_copy(others, others, rm_recv).wait()
    to_scalars = pltpu.make_async_copy(rmap, rmap_s, rm_loc)
    to_scalars.start()
    to_scalars.wait()
    second_tables()
    step(2)

    blocks = psi.shape[1] // 128

    def weigh(s, carry):
        turned = msq[s].T
        for a in range(blocks):
            rows = slice(a * 128, (a + 1) * 128)
            wgt[s, rows, :] = (turned[:, a:a + 1] * psi[s, rows, :].astype(jnp.float32)).astype(jnp.bfloat16)
        return carry

    msq[...] = jnp.zeros_like(msq)
    loads["mass"].wait()
    for s in range(count):
        for a in range(blocks):
            msq[s, a:a + 1, :] = mass[s:s + 1, a * 128:(a + 1) * 128]
    lax.fori_loop(0, count, weigh, 0)

    step(3)
    loads["mbb"].wait()
    mass_block(0, reds[3])
    for c in (6, 7, 8):
        send_lanes(c)
    step(4)
    mass_block(1, reds[4])
    for c in (9, 10):
        send_lanes(c)
    step(5)
    mass_block(2, reds[5])
    send_lanes(11)
    step(6)

    def settle(r, carry):
        starts = [rmap_s[r, 0, 3 * j] - me * BPO for j in range(group)]
        which = jnp.int32(-1)
        for j, start in enumerate(starts):
            which = jnp.where((start >= 0) & (start < BPO), j, which)
        spot = 3 * jnp.maximum(which, 0)
        found = [jnp.where(which >= 0, rmap_s[r, 0, spot + i] - me * BPO, -1) for i in range(3)]
        table[pl.ds(r, 1)] = as_row(found, 0)
        return carry

    lax.fori_loop(0, owners, settle, 0)
    loads["fix"].wait()

    def couple(s, carry):
        coup[s] = lax.dot_general(fix[s], wgt[s], (((0,), (0,)), ((), ())), preferred_element_type=jnp.float32)
        return carry

    step(7)
    lax.fori_loop(0, 1, couple, 0)
    step(8)
    lax.fori_loop(1, 2, couple, 0)
    step(9)
    lax.fori_loop(2, count, couple, 0)
    coup_copy = pltpu.make_async_copy(coup, coup_hbm, coup_sem)
    coup_copy.start()
    table_copy = pltpu.make_async_copy(table, table_hbm, table_sem)
    table_copy.start()
    for c in range(10, n_chunks + LAGS[1]):
        step(c)

    coup_copy.wait()
    table_copy.wait()
    for d in range(1, lanes):
        map_sends[d - 1].wait_send()
    pltpu.make_async_copy(others, others, rm_send).wait()
    for copies in (z_copies, f_copies, p_copies):
        for copy in copies.values():
            copy.wait_send()
    for c in range(n_chunks):
        for h in range(2):
            own_copy(c, h).wait()
            sent = seconds[c].at[h, pl.ds(4, 28)]
            pltpu.make_async_copy(sent, sent, x_send.at[c, h]).wait()
            pltpu.make_async_copy(sent, sent, x_recv.at[c, h]).wait()


def assemble(
    owners, table_hbm, recv0_hbm, recv1_hbm, coup_hbm, k_hbm, m_hbm, coup_out,
    table, buf0, buf1, k_acc, m_acc, coup, table_sem, in_sem, out_sem, coup_in, coup_back,
):
    me = lax.axis_index("row")
    pairs = len(PAIRS)
    half = buf0.shape[2]
    to_scalars = pltpu.make_async_copy(table_hbm, table, table_sem)
    to_scalars.start()

    def begin(mat):
        def one(q, carry):
            slots, planes = pl.ds(q * 4, 4), pl.ds(mat * pairs, pairs)
            for src, dst, h in ((recv0_hbm, buf0, 0), (recv1_hbm, buf1, 1)):
                pltpu.make_async_copy(src.at[slots, planes], dst.at[slots, planes], in_sem.at[mat, h]).start()
            return carry

        lax.fori_loop(0, owners // 4, one, 0)

    def ready(mat):
        planes = pl.ds(mat * pairs, pairs)
        for src, dst, h in ((recv0_hbm, buf0, 0), (recv1_hbm, buf1, 1)):
            pltpu.make_async_copy(src.at[:, planes], dst.at[:, planes], in_sem.at[mat, h]).wait()

    begin(0)
    begin(1)
    take = pltpu.make_async_copy(coup_hbm, coup, coup_in)
    take.start()

    def clear(e, carry):
        k_acc[e] = jnp.zeros(k_acc.shape[1:], jnp.float32)
        m_acc[e] = jnp.zeros(m_acc.shape[1:], jnp.float32)
        return carry

    lax.fori_loop(0, BPO * BAND, clear, 0)
    to_scalars.wait()

    def add(acc, mat):
        def one(r, carry):
            places = [table[r, 0, i] for i in range(3)]
            y, x, k = r // 8, (r // 2) % 4, r % 2
            spots = ((x * 2 + k) * 4 + (me // 8 + 4 - y) % 4, (y * 2 + k) * 4 + ((me // 2) % 4 + 4 - x) % 4)

            @pl.when(places[0] >= 0)
            def _():
                entries = [places[i] * BAND + places[j] - places[i] for i, j in PAIRS]
                sums = [
                    acc[e, h * half:(h + 1) * half, :] + buf[spots[h], mat * pairs + p]
                    for p, e in enumerate(entries) for h, buf in enumerate((buf0, buf1))
                ]
                for i, total in enumerate(sums):
                    h = i % 2
                    acc[entries[i // 2], h * half:(h + 1) * half, :] = total

            return carry

        lax.fori_loop(0, owners, one, 0)

    ready(0)
    add(k_acc, 0)
    k_out = pltpu.make_async_copy(k_acc, k_hbm, out_sem.at[0])
    k_out.start()
    take.wait()
    give = pltpu.make_async_copy(coup, coup_out, coup_back)
    give.start()
    ready(1)
    add(m_acc, 1)
    m_out = pltpu.make_async_copy(m_acc, m_hbm, out_sem.at[1])
    m_out.start()
    k_out.wait()
    give.wait()
    m_out.wait()


def per_device(stiff_bb, stiff_bi, constraint_modes, interior_mass, fixed_modes, mass_bb, boundary_map):
    owners, lanes = lax.axis_size("row"), lax.axis_size("col")
    count, inner, order = constraint_modes.shape
    modes = fixed_modes.shape[2]
    width = order // 3
    part = width // lanes
    half = part // 2
    group = lanes * count
    planes = 2 * len(PAIRS)

    anywhere = pl.BlockSpec(memory_space=pl.ANY)
    f32, bf16, i32 = jnp.float32, jnp.bfloat16, jnp.int32
    dma = pltpu.SemaphoreType.DMA
    received0, received1, table, coupling = pl.pallas_call(
        functools.partial(reduce_and_send, owners, lanes),
        out_shape=(
            jax.ShapeDtypeStruct((owners, planes, half, width), f32),
            jax.ShapeDtypeStruct((owners, planes, half, width), f32),
            jax.ShapeDtypeStruct((owners, 1, 128), i32),
            jax.ShapeDtypeStruct((count, modes, order), f32),
        ),
        in_specs=[anywhere] * 7,
        out_specs=(anywhere,) * 4,
        scratch_shapes=[
            pltpu.VMEM((count, inner, order), bf16),
            pltpu.VMEM((count, order, inner), bf16),
            pltpu.VMEM((count, inner, modes), bf16),
            pltpu.VMEM((count, inner, order), bf16),
            pltpu.VMEM((count, 3, width, order), bf16),
            pltpu.VMEM((count, 3, width, order), bf16),
            pltpu.VMEM((count, inner), f32),
            pltpu.VMEM((count, 128, 128), f32),
            pltpu.VMEM((count, modes, order), f32),
            pltpu.SMEM((count, 3), i32),
            pltpu.VMEM((1, 1, 128), i32),
            pltpu.VMEM((lanes, 1, 128), i32),
            pltpu.VMEM((1, 1, 128), i32),
            pltpu.SMEM((1, 1, 128), i32),
            pltpu.VMEM((owners, 1, 128), i32),
            pltpu.SMEM((owners, 1, 128), i32),
            pltpu.SMEM((32,), i32),
            pltpu.SMEM((64,), i32),
            pltpu.VMEM((owners, 1, 128), i32),
        ]
        + [pltpu.VMEM((count, 3 - b, width, width), f32) for _, b in BLOCKS]
        + [pltpu.VMEM((group, 2, half, width), f32)] * len(CHUNKS)
        + [pltpu.VMEM((2, 16, half, width), f32)] * len(CHUNKS)
        + [pltpu.VMEM((2, 24, half, width), f32)] * len(CHUNKS)
        + [pltpu.VMEM((2, 32, half, width), f32)] * len(CHUNKS)
        + [
            dma((13,)), dma, dma, dma((lanes - 1,)), dma((lanes - 1,)), dma, dma, dma, dma,
            dma((len(CHUNKS), 2, lanes - 1)), dma((len(CHUNKS), 2, lanes - 1)),
            dma((len(CHUNKS), 2, 2)), dma((len(CHUNKS), 2, 2)), dma((len(CHUNKS), 2, 2)), dma((len(CHUNKS), 2, 2)),
            dma((len(CHUNKS), 2)), dma((len(CHUNKS), 2)), dma((len(CHUNKS), 2)),
        ],
        compiler_params=pltpu.CompilerParams(
            collective_id=0, has_side_effects=True, vmem_limit_bytes=60 * 1024 * 1024),
        name="reduce_and_send",
    )(boundary_map, interior_mass, stiff_bb, stiff_bi, constraint_modes, fixed_modes, mass_bb)

    entry = (BPO * BAND, part, width)
    in_hbm = pl.BlockSpec(memory_space=pltpu.HBM)
    k_band, m_band, coupling = pl.pallas_call(
        functools.partial(assemble, owners),
        out_shape=(
            jax.ShapeDtypeStruct(entry, f32),
            jax.ShapeDtypeStruct(entry, f32),
            jax.ShapeDtypeStruct((count, modes, order), f32),
        ),
        in_specs=[in_hbm] * 4,
        out_specs=[in_hbm] * 3,
        scratch_shapes=[
            pltpu.SMEM((owners, 1, 128), i32),
            pltpu.VMEM((owners, planes, half, width), f32),
            pltpu.VMEM((owners, planes, half, width), f32),
            pltpu.VMEM(entry, f32),
            pltpu.VMEM(entry, f32),
            pltpu.VMEM((count, modes, order), f32),
            dma, dma((2, 2)), dma((2,)), dma, dma,
        ],
        compiler_params=pltpu.CompilerParams(vmem_limit_bytes=60 * 1024 * 1024),
        name="assemble",
    )(table, received0, received1, coupling)
    banded = (BPO, BAND, part, width)
    return k_band.reshape(banded), m_band.reshape(banded), coupling


def solution(mesh):
    both = ("row", "col")
    return jax.shard_map(
        per_device,
        mesh=mesh,
        in_specs=(
            P(both, None, None, None), P(both, None, None), P(both, None, None), P(both, None),
            P(both, None, None), P(both, None, None, None), P(both, None),
        ),
        out_specs=(P("row", None, "col", None), P("row", None, "col", None), P(both, None, None)),
        check_vma=False,
    )
```

```python
import functools

import jax
import jax.numpy as jnp
from jax import lax
from jax.experimental import pallas as pl
from jax.experimental.pallas import tpu as pltpu
from jax.sharding import PartitionSpec as P

BAND = 4
LAGS = (1, 3)
BPO = 24
MESH = pl.DeviceIdType.MESH

PAIRS = ((2, 2), (1, 1), (1, 2), (0, 0), (0, 1), (0, 2))
BLOCKS = ((0, 2), (0, 1), (0, 0), (1, 0), (1, 1), (1, 2))
CHUNKS = tuple(
    (i, q, mat * len(PAIRS) + (0, 1, 3)[2 - b] + q) for i, (mat, b) in enumerate(BLOCKS) for q in range(3 - b)
)


def row_of(y, x, k):
    return y * 8 + x * 2 + k


def place(h, f, g, k):
    return row_of(f, g, k) if h == 0 else row_of(g, f, k)


def owner_of(block):
    return lax.shift_right_logical(block * 2731, jnp.int32(16))


def first_axis(h, owner):
    return lax.shift_right_logical(owner, jnp.int32(3)) if h == 0 else lax.shift_right_logical(owner, jnp.int32(1)) & 3


def count_before(flags):
    total, before = jnp.int32(0), []
    for flag in flags:
        before.append(total)
        total = total + jnp.where(flag, 1, 0)
    return before, total


def find(keys, values, wanted):
    found = jnp.int32(0)
    for key, value in zip(keys, values):
        found = jnp.where(key == wanted, value, found)
    return found


def reduce_and_send(
    owners, lanes,
    map_hbm, mass_hbm, sbb_hbm, sbi_hbm, psi_hbm, fix_hbm, mbb_hbm,
    recv0_hbm, recv1_hbm, table_hbm, coup_hbm,
    psi, sbi, fix, wgt, sbb, mbb, mass, msq, coup, map_s, mine, zmap, whole, whole_s, rmap, rmap_s, pick1, pick2, table,
    *rest,
):
    n_chunks = len(CHUNKS)
    reds, rest = rest[:len(BLOCKS)], rest[len(BLOCKS):]
    zs, firsts, arrived, seconds = (rest[i * n_chunks:(i + 1) * n_chunks] for i in range(4))
    (in_sem, coup_sem, table_sem, zm_send, zm_recv, zm_loc, rm_send, rm_recv, rm_loc,
     z_send, z_recv, f_send, f_recv, p_send, p_recv, x_send, x_recv, x_own) = rest[4 * n_chunks:]
    recvs = (recv0_hbm, recv1_hbm)
    me, lane = lax.axis_index("row"), lax.axis_index("col")
    y, x, core = me // 8, (me // 2) % 4, me % 2
    at = [(y, x), (x, y)]
    beside = [[place(h, (f + step) % 4, g, core) for step in (1, 3)] for h, (f, g) in enumerate(at)]
    line = [[place(h, f, (g + t // 2) % 4, (core + t) % 2) for t in range(8)] for h, (f, g) in enumerate(at)]
    from_here = [pl.ds((g * 2 + core) * 4, 4) for _, g in at]
    count, order = psi.shape[0], psi.shape[2]
    width = order // 3
    part = width // lanes
    half = part // 2
    group = lanes * count

    loads = {}

    def load(name, src, dst):
        loads[name] = pltpu.make_async_copy(src, dst, in_sem.at[len(loads)])
        loads[name].start()

    def load_block(b):
        cols = pl.ds(b * width, width)
        load(("psi", b), psi_hbm.at[:, :, cols], psi.at[:, :, cols])
        load(("sbi", b), sbi_hbm.at[:, cols, :], sbi.at[:, cols, :])
        load(("sbb", b), sbb_hbm.at[:, b], sbb.at[:, b])

    def loaded(b):
        for name in ("psi", "sbi", "sbb"):
            loads[name, b].wait()

    load("map", map_hbm, map_s)
    load_block(2)

    barrier = pltpu.get_barrier_semaphore()
    for d in range(1, lanes):
        pl.semaphore_signal(barrier, inc=1, device_id=(me, lax.rem(lane + d, lanes)), device_id_type=MESH)

    def greet(t, carry):
        pl.semaphore_signal(barrier, inc=1, device_id=(lax.rem(me + t, owners), lane), device_id_type=MESH)
        return carry

    lax.fori_loop(1, owners, greet, 0)

    loads["map"].wait()
    lanes_of = lax.broadcasted_iota(jnp.int32, (1, 1, 128), 2)

    def as_row(scalars, offset):
        row = jnp.zeros((1, 1, 128), jnp.int32)
        for i, scalar in enumerate(scalars):
            row = jnp.where(lanes_of == offset + i, scalar, row)
        return row

    own = as_row([map_s[s, i] for s in range(count) for i in range(3)], 3 * count * lane)
    mine[...] = own
    zmap[pl.ds(lane, 1)] = own

    def stiff_block(b, red):
        n = 3 - b

        def one(s, carry):
            out = jnp.dot(sbi[s, pl.ds(b * width, width), :], psi[s, :, pl.ds(b * width, n * width)],
                          preferred_element_type=jnp.float32)
            out = out + sbb[s, b, :, pl.ds(b * width, n * width)].astype(jnp.float32)
            for q in range(n):
                red[s, q] = out[:, q * width:(q + 1) * width]
            return carry

        lax.fori_loop(0, count, one, 0)

    def mass_block(b, red):
        n = 3 - b

        def one(s, carry):
            out = lax.dot_general(psi[s, :, pl.ds(b * width, width)], wgt[s, :, pl.ds(b * width, n * width)],
                                  (((0,), (0,)), ((), ())), preferred_element_type=jnp.float32)
            out = out + mbb[s, b, :, pl.ds(b * width, n * width)].astype(jnp.float32)
            for q in range(n):
                red[s, q] = out[:, q * width:(q + 1) * width]
            return carry

        lax.fori_loop(0, count, one, 0)

    z_copies, f_copies, p_copies = {}, {}, {}

    def send_lanes(c):
        red, q, z = reds[CHUNKS[c][0]], CHUNKS[c][1], zs[c]
        ours = pl.ds(count * lane, count)
        for h in range(2):
            z[ours, h] = red[:, q, pl.ds(pl.multiple_of(part * lane + half * h, half), half), :]
        for d in range(1, lanes):
            peer = lax.rem(lane + d, lanes)
            for h in range(2):
                copy = pltpu.make_async_remote_copy(
                    src_ref=red.at[:, q, pl.ds(pl.multiple_of(part * peer + half * h, half), half), :],
                    dst_ref=z.at[ours, h], send_sem=z_send.at[c, h, d - 1],
                    recv_sem=z_recv.at[c, h, d - 1], device_id=(me, peer), device_id_type=MESH)
                copy.start()
                z_copies[c, h, d] = copy

    def first_leg(c):
        z, first = zs[c], firsts[c]
        for copy in [z_copies[c, h, d] for h in range(2) for d in range(1, lanes)]:
            copy.wait_recv()
        for h in range(2):
            slots = [z[pick1[h * 16 + t], h] for t in range(16)]
            for t in range(16):
                first[h, t] = slots[t]
        for h in range(2):
            for way in range(2):
                copy = pltpu.make_async_remote_copy(
                    src_ref=first.at[h, pl.ds(8 * way, 8)], dst_ref=arrived[c].at[h, pl.ds(8 * way, 8)],
                    send_sem=f_send.at[c, h, way], recv_sem=f_recv.at[c, h, way],
                    device_id=(beside[h][way], lane), device_id_type=MESH)
                copy.start()
                f_copies[c, h, way] = copy

    def pass_on(c):
        for h in range(2):
            for way in range(2):
                f_copies[c, h, way].wait_recv()
                copy = pltpu.make_async_remote_copy(
                    src_ref=arrived[c].at[h, pl.ds(8 * way + 4, 4)], dst_ref=arrived[c].at[h, pl.ds(16 + 4 * way, 4)],
                    send_sem=p_send.at[c, h, way], recv_sem=p_recv.at[c, h, way],
                    device_id=(beside[h][way], lane), device_id_type=MESH)
                copy.start()
                p_copies[c, h, way] = copy

    def own_copy(c, h):
        return pltpu.make_async_copy(
            seconds[c].at[h, pl.ds(0, 4)], recvs[h].at[from_here[h], CHUNKS[c][2]], x_own.at[c, h])

    def second_leg(c):
        z, second = zs[c], seconds[c]
        for copy in [p_copies[c, h, way] for h in range(2) for way in range(2)]:
            copy.wait_recv()
        for h in range(2):
            for low in (0, 16):
                picked = [
                    z[pick2[h * 32 + i], h] if i % 4 == 0 else arrived[c][h, pick2[h * 32 + i]]
                    for i in range(low, low + 16)
                ]
                for i, value in enumerate(picked):
                    second[h, low + i] = value
            own_copy(c, h).start()
        for t in range(1, 8):
            for h in range(2):
                pltpu.make_async_remote_copy(
                    src_ref=second.at[h, pl.ds(t * 4, 4)], dst_ref=recvs[h].at[from_here[h], CHUNKS[c][2]],
                    send_sem=x_send.at[c, h], recv_sem=x_recv.at[c, h],
                    device_id=(line[h][t], lane), device_id_type=MESH).start()

    def first_tables():
        heads = [owner_of(whole_s[0, 0, 3 * j]) for j in range(group)]
        numbers = [jnp.int32(j) for j in range(group)]
        for h in range(2):
            f = at[h][0]
            away = [(first_axis(h, head) + 4 - f) & 3 for head in heads]
            near, n1 = count_before([a == 1 for a in away])
            far, n2 = count_before([a == 2 for a in away])
            back, _ = count_before([a == 3 for a in away])
            split = jnp.minimum(jnp.minimum(n2, 8 - n1), 4)
            plus = [jnp.where(a == 1, r1, jnp.where((a == 2) & (r2 < split), 7 - r2, -1))
                    for a, r1, r2 in zip(away, near, far)]
            minus = [jnp.where(a == 3, r3, jnp.where((a == 2) & (r2 >= split), 7 + split - r2, -1))
                     for a, r3, r2 in zip(away, back, far)]
            for t in range(8):
                pick1[h * 16 + t] = find(plus, numbers, t)
                pick1[h * 16 + 8 + t] = find(minus, numbers, t)
            for t in range(8):
                pick2[h * 32 + t * 4] = find(heads, numbers, line[h][t])

    def second_tables():
        for h in range(2):
            f, g = at[h]
            for d in range(1, 4):
                source = place(h, (f + 4 - d) % 4, g, core)
                heads = [owner_of(rmap_s[source, 0, 3 * j]) for j in range(group)]
                axis = [first_axis(h, head) for head in heads]
                rank, n2 = count_before([a == f for a in axis])
                if d == 1:
                    spot = rank
                elif d == 3:
                    spot = [8 + r for r in rank]
                else:
                    _, n1 = count_before([a == (f + 3) % 4 for a in axis])
                    split = jnp.minimum(jnp.minimum(n2, 8 - n1), 4)
                    spot = [jnp.where(r < split, 19 - r, 23 + split - r) for r in rank]
                for t in range(8):
                    pick2[h * 32 + t * 4 + d] = find(heads, spot, line[h][t])

    def step(c):
        if c < n_chunks:
            first_leg(c)
        if 0 <= c - LAGS[0] < n_chunks:
            pass_on(c - LAGS[0])
        if 0 <= c - LAGS[1] < n_chunks:
            second_leg(c - LAGS[1])

    loaded(2)
    load_block(1)
    stiff_block(2, reds[0])
    pl.semaphore_wait(barrier, owners + lanes - 2)
    map_sends = []
    for d in range(1, lanes):
        peer = lax.rem(lane + d, lanes)
        copy = pltpu.make_async_remote_copy(
            src_ref=mine, dst_ref=zmap.at[pl.ds(lane, 1)], send_sem=zm_send.at[d - 1],
            recv_sem=zm_recv.at[d - 1], device_id=(me, peer), device_id_type=MESH)
        copy.start()
        map_sends.append(copy)
    send_lanes(0)
    loaded(1)
    load_block(0)
    stiff_block(1, reds[1])
    send_lanes(1)
    send_lanes(2)

    for d in range(1, lanes):
        map_sends[d - 1].wait_recv()
    merged = zmap[0:1]
    for i in range(1, lanes):
        merged = merged + zmap[i:i + 1]
    whole[...] = merged
    rmap[pl.ds(me, 1)] = merged
    to_scalars = pltpu.make_async_copy(whole, whole_s, zm_loc)
    to_scalars.start()

    to_scalars.wait()
    first_tables()
    step(0)

    def tell(t, carry):
        pltpu.make_async_remote_copy(
            src_ref=whole, dst_ref=rmap.at[pl.ds(me, 1)], send_sem=rm_send, recv_sem=rm_recv,
            device_id=(lax.rem(me + t, owners), lane), device_id_type=MESH).start()
        return carry

    lax.fori_loop(1, owners, tell, 0)
    loaded(0)
    load("mass", mass_hbm, mass)
    load("mbb", mbb_hbm, mbb)
    load("fix", fix_hbm, fix)
    stiff_block(0, reds[2])
    for c in (3, 4, 5):
        send_lanes(c)
    step(1)

    others = rmap.at[pl.ds(0, owners - 1)]
    pltpu.make_async_copy(others, others, rm_recv).wait()
    to_scalars = pltpu.make_async_copy(rmap, rmap_s, rm_loc)
    to_scalars.start()
    to_scalars.wait()
    second_tables()
    step(2)

    blocks = psi.shape[1] // 128

    def weigh(s, carry):
        turned = msq[s].T
        for a in range(blocks):
            rows = slice(a * 128, (a + 1) * 128)
            wgt[s, rows, :] = (turned[:, a:a + 1] * psi[s, rows, :].astype(jnp.float32)).astype(jnp.bfloat16)
        return carry

    msq[...] = jnp.zeros_like(msq)
    loads["mass"].wait()
    for s in range(count):
        for a in range(blocks):
            msq[s, a:a + 1, :] = mass[s:s + 1, a * 128:(a + 1) * 128]
    lax.fori_loop(0, count, weigh, 0)

    step(3)
    loads["mbb"].wait()
    mass_block(0, reds[3])
    for c in (6, 7, 8):
        send_lanes(c)
    step(4)
    mass_block(1, reds[4])
    for c in (9, 10):
        send_lanes(c)
    step(5)
    mass_block(2, reds[5])
    send_lanes(11)
    step(6)

    def settle(r, carry):
        starts = [rmap_s[r, 0, 3 * j] - me * BPO for j in range(group)]
        which = jnp.int32(-1)
        for j, start in enumerate(starts):
            which = jnp.where((start >= 0) & (start < BPO), j, which)
        spot = 3 * jnp.maximum(which, 0)
        at_home = [rmap_s[r, 0, spot + i] - me * BPO for i in range(3)]
        found = [
            jnp.where(which >= 0, at_home[i] * BAND + at_home[j] - at_home[i], BPO * BAND) for i, j in PAIRS
        ]
        table[pl.ds(r, 1)] = as_row(found, 0)
        return carry

    lax.fori_loop(0, owners, settle, 0)
    loads["fix"].wait()

    def couple(s, carry):
        coup[s] = lax.dot_general(fix[s], wgt[s], (((0,), (0,)), ((), ())), preferred_element_type=jnp.float32)
        return carry

    step(7)
    lax.fori_loop(0, 1, couple, 0)
    step(8)
    lax.fori_loop(1, 2, couple, 0)
    step(9)
    lax.fori_loop(2, count, couple, 0)
    coup_copy = pltpu.make_async_copy(coup, coup_hbm, coup_sem)
    coup_copy.start()
    table_copy = pltpu.make_async_copy(table, table_hbm, table_sem)
    table_copy.start()
    for c in range(10, n_chunks + LAGS[1]):
        step(c)

    coup_copy.wait()
    table_copy.wait()
    for d in range(1, lanes):
        map_sends[d - 1].wait_send()
    pltpu.make_async_copy(others, others, rm_send).wait()
    for copies in (z_copies, f_copies, p_copies):
        for copy in copies.values():
            copy.wait_send()
    for c in range(n_chunks):
        for h in range(2):
            own_copy(c, h).wait()
            sent = seconds[c].at[h, pl.ds(4, 28)]
            pltpu.make_async_copy(sent, sent, x_send.at[c, h]).wait()
            pltpu.make_async_copy(sent, sent, x_recv.at[c, h]).wait()


def assemble(
    owners, table_hbm, recv0_hbm, recv1_hbm, coup_hbm, k_hbm, m_hbm, coup_out,
    table, buf0, buf1, k_acc, m_acc, coup, table_sem, in_sem, out_sem, coup_in, coup_back,
):
    me = lax.axis_index("row")
    pairs = len(PAIRS)
    half = buf0.shape[2]
    to_scalars = pltpu.make_async_copy(table_hbm, table, table_sem)
    to_scalars.start()

    def begin(mat):
        def one(q, carry):
            slots, planes = pl.ds(q * 4, 4), pl.ds(mat * pairs, pairs)
            for src, dst, h in ((recv0_hbm, buf0, 0), (recv1_hbm, buf1, 1)):
                pltpu.make_async_copy(src.at[slots, planes], dst.at[slots, planes], in_sem.at[mat, h]).start()
            return carry

        lax.fori_loop(0, owners // 4, one, 0)

    def ready(mat):
        planes = pl.ds(mat * pairs, pairs)
        for src, dst, h in ((recv0_hbm, buf0, 0), (recv1_hbm, buf1, 1)):
            pltpu.make_async_copy(src.at[:, planes], dst.at[:, planes], in_sem.at[mat, h]).wait()

    begin(0)
    begin(1)
    take = pltpu.make_async_copy(coup_hbm, coup, coup_in)
    take.start()

    def clear(e, carry):
        k_acc[e] = jnp.zeros(k_acc.shape[1:], jnp.float32)
        m_acc[e] = jnp.zeros(m_acc.shape[1:], jnp.float32)
        return carry

    lax.fori_loop(0, BPO * BAND + 1, clear, 0)
    to_scalars.wait()

    def add(acc, mat):
        def one(y, carry):
            for g in range(4):
                for k in range(2):
                    r = y * 8 + g * 2 + k
                    spots = ((g * 2 + k) * 4 + (me // 8 + 4 - y) % 4, (y * 2 + k) * 4 + (me // 2 + 4 - g) % 4)
                    entries = [table[r, 0, p] for p in range(pairs)]
                    sums = [
                        acc[e, h * half:(h + 1) * half, :] + buf[spots[h], mat * pairs + p]
                        for p, e in enumerate(entries) for h, buf in enumerate((buf0, buf1))
                    ]
                    for i, total in enumerate(sums):
                        h = i % 2
                        acc[entries[i // 2], h * half:(h + 1) * half, :] = total
            return carry

        lax.fori_loop(0, 4, one, 0)

    ready(0)
    add(k_acc, 0)
    k_out = pltpu.make_async_copy(k_acc.at[pl.ds(0, BPO * BAND)], k_hbm, out_sem.at[0])
    k_out.start()
    take.wait()
    give = pltpu.make_async_copy(coup, coup_out, coup_back)
    give.start()
    ready(1)
    add(m_acc, 1)
    m_out = pltpu.make_async_copy(m_acc.at[pl.ds(0, BPO * BAND)], m_hbm, out_sem.at[1])
    m_out.start()
    k_out.wait()
    give.wait()
    m_out.wait()


def per_device(stiff_bb, stiff_bi, constraint_modes, interior_mass, fixed_modes, mass_bb, boundary_map):
    owners, lanes = lax.axis_size("row"), lax.axis_size("col")
    count, inner, order = constraint_modes.shape
    modes = fixed_modes.shape[2]
    width = order // 3
    part = width // lanes
    half = part // 2
    group = lanes * count
    planes = 2 * len(PAIRS)

    anywhere = pl.BlockSpec(memory_space=pl.ANY)
    f32, bf16, i32 = jnp.float32, jnp.bfloat16, jnp.int32
    dma = pltpu.SemaphoreType.DMA
    received0, received1, table, coupling = pl.pallas_call(
        functools.partial(reduce_and_send, owners, lanes),
        out_shape=(
            jax.ShapeDtypeStruct((owners, planes, half, width), f32),
            jax.ShapeDtypeStruct((owners, planes, half, width), f32),
            jax.ShapeDtypeStruct((owners, 1, 128), i32),
            jax.ShapeDtypeStruct((count, modes, order), f32),
        ),
        in_specs=[anywhere] * 7,
        out_specs=(anywhere,) * 4,
        scratch_shapes=[
            pltpu.VMEM((count, inner, order), bf16),
            pltpu.VMEM((count, order, inner), bf16),
            pltpu.VMEM((count, inner, modes), bf16),
            pltpu.VMEM((count, inner, order), bf16),
            pltpu.VMEM((count, 3, width, order), bf16),
            pltpu.VMEM((count, 3, width, order), bf16),
            pltpu.VMEM((count, inner), f32),
            pltpu.VMEM((count, 128, 128), f32),
            pltpu.VMEM((count, modes, order), f32),
            pltpu.SMEM((count, 3), i32),
            pltpu.VMEM((1, 1, 128), i32),
            pltpu.VMEM((lanes, 1, 128), i32),
            pltpu.VMEM((1, 1, 128), i32),
            pltpu.SMEM((1, 1, 128), i32),
            pltpu.VMEM((owners, 1, 128), i32),
            pltpu.SMEM((owners, 1, 128), i32),
            pltpu.SMEM((32,), i32),
            pltpu.SMEM((64,), i32),
            pltpu.VMEM((owners, 1, 128), i32),
        ]
        + [pltpu.VMEM((count, 3 - b, width, width), f32) for _, b in BLOCKS]
        + [pltpu.VMEM((group, 2, half, width), f32)] * len(CHUNKS)
        + [pltpu.VMEM((2, 16, half, width), f32)] * len(CHUNKS)
        + [pltpu.VMEM((2, 24, half, width), f32)] * len(CHUNKS)
        + [pltpu.VMEM((2, 32, half, width), f32)] * len(CHUNKS)
        + [
            dma((13,)), dma, dma, dma((lanes - 1,)), dma((lanes - 1,)), dma, dma, dma, dma,
            dma((len(CHUNKS), 2, lanes - 1)), dma((len(CHUNKS), 2, lanes - 1)),
            dma((len(CHUNKS), 2, 2)), dma((len(CHUNKS), 2, 2)), dma((len(CHUNKS), 2, 2)), dma((len(CHUNKS), 2, 2)),
            dma((len(CHUNKS), 2)), dma((len(CHUNKS), 2)), dma((len(CHUNKS), 2)),
        ],
        compiler_params=pltpu.CompilerParams(
            collective_id=0, has_side_effects=True, vmem_limit_bytes=60 * 1024 * 1024),
        name="reduce_and_send",
    )(boundary_map, interior_mass, stiff_bb, stiff_bi, constraint_modes, fixed_modes, mass_bb)

    entry = (BPO * BAND, part, width)
    in_hbm = pl.BlockSpec(memory_space=pltpu.HBM)
    k_band, m_band, coupling = pl.pallas_call(
        functools.partial(assemble, owners),
        out_shape=(
            jax.ShapeDtypeStruct(entry, f32),
            jax.ShapeDtypeStruct(entry, f32),
            jax.ShapeDtypeStruct((count, modes, order), f32),
        ),
        in_specs=[in_hbm] * 4,
        out_specs=[in_hbm] * 3,
        scratch_shapes=[
            pltpu.SMEM((owners, 1, 128), i32),
            pltpu.VMEM((owners, planes, half, width), f32),
            pltpu.VMEM((owners, planes, half, width), f32),
            pltpu.VMEM((BPO * BAND + 1, part, width), f32),
            pltpu.VMEM((BPO * BAND + 1, part, width), f32),
            pltpu.VMEM((count, modes, order), f32),
            dma, dma((2, 2)), dma((2,)), dma, dma,
        ],
        compiler_params=pltpu.CompilerParams(vmem_limit_bytes=60 * 1024 * 1024),
        name="assemble",
    )(table, received0, received1, coupling)
    banded = (BPO, BAND, part, width)
    return k_band.reshape(banded), m_band.reshape(banded), coupling


def solution(mesh):
    both = ("row", "col")
    return jax.shard_map(
        per_device,
        mesh=mesh,
        in_specs=(
            P(both, None, None, None), P(both, None, None), P(both, None, None), P(both, None),
            P(both, None, None), P(both, None, None, None), P(both, None),
        ),
        out_specs=(P("row", None, "col", None), P("row", None, "col", None), P(both, None, None)),
        check_vma=False,
    )
```

```python
import functools

import jax
import jax.numpy as jnp
from jax import lax
from jax.experimental import pallas as pl
from jax.experimental.pallas import tpu as pltpu
from jax.sharding import PartitionSpec as P

BAND = 4
LAGS = (1, 3)
BPO = 24
MESH = pl.DeviceIdType.MESH

PAIRS = ((2, 2), (1, 1), (1, 2), (0, 0), (0, 1), (0, 2))
BLOCKS = ((0, 2), (0, 1), (0, 0), (1, 0), (1, 1), (1, 2))
CHUNKS = tuple(
    (i, q, mat * len(PAIRS) + (0, 1, 3)[2 - b] + q) for i, (mat, b) in enumerate(BLOCKS) for q in range(3 - b)
)


def row_of(y, x, k):
    return y * 8 + x * 2 + k


def place(h, f, g, k):
    return row_of(f, g, k) if h == 0 else row_of(g, f, k)


def owner_of(block):
    return lax.shift_right_logical(block * 2731, jnp.int32(16))


def first_axis(h, owner):
    return lax.shift_right_logical(owner, jnp.int32(3)) if h == 0 else lax.shift_right_logical(owner, jnp.int32(1)) & 3


def count_before(flags):
    total, before = jnp.int32(0), []
    for flag in flags:
        before.append(total)
        total = total + jnp.where(flag, 1, 0)
    return before, total


def find(keys, values, wanted):
    found = jnp.int32(0)
    for key, value in zip(keys, values):
        found = jnp.where(key == wanted, value, found)
    return found


def reduce_and_send(
    owners, lanes,
    map_hbm, mass_hbm, sbb_hbm, sbi_hbm, psi_hbm, fix_hbm, mbb_hbm,
    recv0_hbm, recv1_hbm, table_hbm, coup_hbm,
    psi, sbi, fix, wgt, sbb, mbb, mass, msq, coup, map_s, mine, zmap, whole, whole_s, rmap, rmap_s, pick1, pick2, table,
    *rest,
):
    n_chunks = len(CHUNKS)
    reds, rest = rest[:len(BLOCKS)], rest[len(BLOCKS):]
    zs, firsts, arrived, seconds = (rest[i * n_chunks:(i + 1) * n_chunks] for i in range(4))
    (in_sem, coup_sem, table_sem, zm_send, zm_recv, zm_loc, rm_send, rm_recv, rm_loc,
     z_send, z_recv, f_send, f_recv, p_send, p_recv, x_send, x_recv, x_own) = rest[4 * n_chunks:]
    recvs = (recv0_hbm, recv1_hbm)
    me, lane = lax.axis_index("row"), lax.axis_index("col")
    y, x, core = me // 8, (me // 2) % 4, me % 2
    at = [(y, x), (x, y)]
    beside = [[place(h, (f + step) % 4, g, core) for step in (1, 3)] for h, (f, g) in enumerate(at)]
    line = [[place(h, f, (g + t // 2) % 4, (core + t) % 2) for t in range(8)] for h, (f, g) in enumerate(at)]
    from_here = [pl.ds((g * 2 + core) * 4, 4) for _, g in at]
    count, order = psi.shape[0], psi.shape[2]
    width = order // 3
    part = width // lanes
    half = part // 2
    group = lanes * count

    loads = {}

    def load(name, src, dst):
        loads[name] = pltpu.make_async_copy(src, dst, in_sem.at[len(loads)])
        loads[name].start()

    def load_block(b):
        cols = pl.ds(b * width, width)
        load(("psi", b), psi_hbm.at[:, :, cols], psi.at[:, :, cols])
        load(("sbi", b), sbi_hbm.at[:, cols, :], sbi.at[:, cols, :])
        load(("sbb", b), sbb_hbm.at[:, b], sbb.at[:, b])

    def loaded(b):
        for name in ("psi", "sbi", "sbb"):
            loads[name, b].wait()

    load("map", map_hbm, map_s)
    load_block(2)

    barrier = pltpu.get_barrier_semaphore()
    for d in range(1, lanes):
        pl.semaphore_signal(barrier, inc=1, device_id=(me, lax.rem(lane + d, lanes)), device_id_type=MESH)

    def greet(t, carry):
        pl.semaphore_signal(barrier, inc=1, device_id=(lax.rem(me + t, owners), lane), device_id_type=MESH)
        return carry

    lax.fori_loop(1, owners, greet, 0)

    loads["map"].wait()
    lanes_of = lax.broadcasted_iota(jnp.int32, (1, 1, 128), 2)

    def as_row(scalars, offset):
        row = jnp.zeros((1, 1, 128), jnp.int32)
        for i, scalar in enumerate(scalars):
            row = jnp.where(lanes_of == offset + i, scalar, row)
        return row

    own = as_row([map_s[s, i] for s in range(count) for i in range(3)], 3 * count * lane)
    mine[...] = own
    zmap[pl.ds(lane, 1)] = own

    def stiff_block(b, red):
        n = 3 - b

        def one(s, carry):
            out = jnp.dot(sbi[s, pl.ds(b * width, width), :], psi[s, :, pl.ds(b * width, n * width)],
                          preferred_element_type=jnp.float32)
            out = out + sbb[s, b, :, pl.ds(b * width, n * width)].astype(jnp.float32)
            for q in range(n):
                red[s, q] = out[:, q * width:(q + 1) * width]
            return carry

        lax.fori_loop(0, count, one, 0)

    def mass_block(b, red):
        n = 3 - b

        def one(s, carry):
            out = lax.dot_general(psi[s, :, pl.ds(b * width, width)], wgt[s, :, pl.ds(b * width, n * width)],
                                  (((0,), (0,)), ((), ())), preferred_element_type=jnp.float32)
            out = out + mbb[s, b, :, pl.ds(b * width, n * width)].astype(jnp.float32)
            for q in range(n):
                red[s, q] = out[:, q * width:(q + 1) * width]
            return carry

        lax.fori_loop(0, count, one, 0)

    z_copies, f_copies, p_copies = {}, {}, {}

    def send_lanes(c):
        red, q, z = reds[CHUNKS[c][0]], CHUNKS[c][1], zs[c]
        ours = pl.ds(count * lane, count)
        for h in range(2):
            z[ours, h] = red[:, q, pl.ds(pl.multiple_of(part * lane + half * h, half), half), :]
        for d in range(1, lanes):
            peer = lax.rem(lane + d, lanes)
            for h in range(2):
                copy = pltpu.make_async_remote_copy(
                    src_ref=red.at[:, q, pl.ds(pl.multiple_of(part * peer + half * h, half), half), :],
                    dst_ref=z.at[ours, h], send_sem=z_send.at[c, h, d - 1],
                    recv_sem=z_recv.at[c, h, d - 1], device_id=(me, peer), device_id_type=MESH)
                copy.start()
                z_copies[c, h, d] = copy

    def first_leg(c):
        z, first = zs[c], firsts[c]
        for copy in [z_copies[c, h, d] for h in range(2) for d in range(1, lanes)]:
            copy.wait_recv()
        for h in range(2):
            slots = [z[pick1[h * 16 + t], h] for t in range(16)]
            for t in range(16):
                first[h, t] = slots[t]
        for h in range(2):
            for way in range(2):
                copy = pltpu.make_async_remote_copy(
                    src_ref=first.at[h, pl.ds(8 * way, 8)], dst_ref=arrived[c].at[h, pl.ds(8 * way, 8)],
                    send_sem=f_send.at[c, h, way], recv_sem=f_recv.at[c, h, way],
                    device_id=(beside[h][way], lane), device_id_type=MESH)
                copy.start()
                f_copies[c, h, way] = copy

    def pass_on(c):
        for h in range(2):
            for way in range(2):
                f_copies[c, h, way].wait_recv()
                copy = pltpu.make_async_remote_copy(
                    src_ref=arrived[c].at[h, pl.ds(8 * way + 4, 4)], dst_ref=arrived[c].at[h, pl.ds(16 + 4 * way, 4)],
                    send_sem=p_send.at[c, h, way], recv_sem=p_recv.at[c, h, way],
                    device_id=(beside[h][way], lane), device_id_type=MESH)
                copy.start()
                p_copies[c, h, way] = copy

    def own_copy(c, h):
        return pltpu.make_async_copy(
            seconds[c].at[h, pl.ds(0, 4)], recvs[h].at[CHUNKS[c][2], from_here[h]], x_own.at[c, h])

    def second_leg(c):
        z, second = zs[c], seconds[c]
        for copy in [p_copies[c, h, way] for h in range(2) for way in range(2)]:
            copy.wait_recv()
        for h in range(2):
            for low in (0, 16):
                picked = [
                    z[pick2[h * 32 + i], h] if i % 4 == 0 else arrived[c][h, pick2[h * 32 + i]]
                    for i in range(low, low + 16)
                ]
                for i, value in enumerate(picked):
                    second[h, low + i] = value
            own_copy(c, h).start()
        for t in (4, 5, 2, 6, 3, 7, 1):
            for h in range(2):
                pltpu.make_async_remote_copy(
                    src_ref=second.at[h, pl.ds(t * 4, 4)], dst_ref=recvs[h].at[CHUNKS[c][2], from_here[h]],
                    send_sem=x_send.at[c, h], recv_sem=x_recv.at[c, h],
                    device_id=(line[h][t], lane), device_id_type=MESH).start()

    def first_tables():
        heads = [owner_of(whole_s[0, 0, 3 * j]) for j in range(group)]
        numbers = [jnp.int32(j) for j in range(group)]
        for h in range(2):
            f = at[h][0]
            away = [(first_axis(h, head) + 4 - f) & 3 for head in heads]
            near, n1 = count_before([a == 1 for a in away])
            far, n2 = count_before([a == 2 for a in away])
            back, _ = count_before([a == 3 for a in away])
            split = jnp.minimum(jnp.minimum(n2, 8 - n1), 4)
            plus = [jnp.where(a == 1, r1, jnp.where((a == 2) & (r2 < split), 7 - r2, -1))
                    for a, r1, r2 in zip(away, near, far)]
            minus = [jnp.where(a == 3, r3, jnp.where((a == 2) & (r2 >= split), 7 + split - r2, -1))
                     for a, r3, r2 in zip(away, back, far)]
            for t in range(8):
                pick1[h * 16 + t] = find(plus, numbers, t)
                pick1[h * 16 + 8 + t] = find(minus, numbers, t)
            for t in range(8):
                pick2[h * 32 + t * 4] = find(heads, numbers, line[h][t])

    def second_tables():
        for h in range(2):
            f, g = at[h]
            for d in range(1, 4):
                source = place(h, (f + 4 - d) % 4, g, core)
                heads = [owner_of(rmap_s[source, 0, 3 * j]) for j in range(group)]
                axis = [first_axis(h, head) for head in heads]
                rank, n2 = count_before([a == f for a in axis])
                if d == 1:
                    spot = rank
                elif d == 3:
                    spot = [8 + r for r in rank]
                else:
                    _, n1 = count_before([a == (f + 3) % 4 for a in axis])
                    split = jnp.minimum(jnp.minimum(n2, 8 - n1), 4)
                    spot = [jnp.where(r < split, 19 - r, 23 + split - r) for r in rank]
                for t in range(8):
                    pick2[h * 32 + t * 4 + d] = find(heads, spot, line[h][t])

    def step(c):
        if c < n_chunks:
            first_leg(c)
        if 0 <= c - LAGS[0] < n_chunks:
            pass_on(c - LAGS[0])
        if 0 <= c - LAGS[1] < n_chunks:
            second_leg(c - LAGS[1])

    loaded(2)
    load_block(1)
    stiff_block(2, reds[0])
    pl.semaphore_wait(barrier, owners + lanes - 2)
    map_sends = []
    for d in range(1, lanes):
        peer = lax.rem(lane + d, lanes)
        copy = pltpu.make_async_remote_copy(
            src_ref=mine, dst_ref=zmap.at[pl.ds(lane, 1)], send_sem=zm_send.at[d - 1],
            recv_sem=zm_recv.at[d - 1], device_id=(me, peer), device_id_type=MESH)
        copy.start()
        map_sends.append(copy)
    send_lanes(0)
    loaded(1)
    load_block(0)
    stiff_block(1, reds[1])
    send_lanes(1)
    send_lanes(2)

    for d in range(1, lanes):
        map_sends[d - 1].wait_recv()
    merged = zmap[0:1]
    for i in range(1, lanes):
        merged = merged + zmap[i:i + 1]
    whole[...] = merged
    rmap[pl.ds(me, 1)] = merged
    to_scalars = pltpu.make_async_copy(whole, whole_s, zm_loc)
    to_scalars.start()

    to_scalars.wait()
    first_tables()
    step(0)

    def tell(t, carry):
        pltpu.make_async_remote_copy(
            src_ref=whole, dst_ref=rmap.at[pl.ds(me, 1)], send_sem=rm_send, recv_sem=rm_recv,
            device_id=(lax.rem(me + t, owners), lane), device_id_type=MESH).start()
        return carry

    lax.fori_loop(1, owners, tell, 0)
    loaded(0)
    load("mass", mass_hbm, mass)
    load("mbb", mbb_hbm, mbb)
    load("fix", fix_hbm, fix)
    stiff_block(0, reds[2])
    for c in (3, 4, 5):
        send_lanes(c)
    step(1)

    others = rmap.at[pl.ds(0, owners - 1)]
    pltpu.make_async_copy(others, others, rm_recv).wait()
    to_scalars = pltpu.make_async_copy(rmap, rmap_s, rm_loc)
    to_scalars.start()
    to_scalars.wait()
    second_tables()
    step(2)

    blocks = psi.shape[1] // 128

    def weigh(s, carry):
        turned = msq[s].T
        for a in range(blocks):
            rows = slice(a * 128, (a + 1) * 128)
            wgt[s, rows, :] = (turned[:, a:a + 1] * psi[s, rows, :].astype(jnp.float32)).astype(jnp.bfloat16)
        return carry

    msq[...] = jnp.zeros_like(msq)
    loads["mass"].wait()
    for s in range(count):
        for a in range(blocks):
            msq[s, a:a + 1, :] = mass[s:s + 1, a * 128:(a + 1) * 128]
    lax.fori_loop(0, count, weigh, 0)

    step(3)
    loads["mbb"].wait()
    mass_block(0, reds[3])
    for c in (6, 7, 8):
        send_lanes(c)
    step(4)
    mass_block(1, reds[4])
    for c in (9, 10):
        send_lanes(c)
    step(5)
    mass_block(2, reds[5])
    send_lanes(11)
    step(6)

    def settle(r, carry):
        starts = [rmap_s[r, 0, 3 * j] - me * BPO for j in range(group)]
        which = jnp.int32(-1)
        for j, start in enumerate(starts):
            which = jnp.where((start >= 0) & (start < BPO), j, which)
        spot = 3 * jnp.maximum(which, 0)
        at_home = [rmap_s[r, 0, spot + i] - me * BPO for i in range(3)]
        found = [
            jnp.where(which >= 0, at_home[i] * BAND + at_home[j] - at_home[i], BPO * BAND) for i, j in PAIRS
        ]
        table[pl.ds(r, 1)] = as_row(found, 0)
        return carry

    lax.fori_loop(0, owners, settle, 0)
    loads["fix"].wait()

    def couple(s, carry):
        coup[s] = lax.dot_general(fix[s], wgt[s], (((0,), (0,)), ((), ())), preferred_element_type=jnp.float32)
        return carry

    step(7)
    lax.fori_loop(0, 1, couple, 0)
    step(8)
    lax.fori_loop(1, 2, couple, 0)
    step(9)
    lax.fori_loop(2, count, couple, 0)
    coup_copy = pltpu.make_async_copy(coup, coup_hbm, coup_sem)
    coup_copy.start()
    table_copy = pltpu.make_async_copy(table, table_hbm, table_sem)
    table_copy.start()
    for c in range(10, n_chunks + LAGS[1]):
        step(c)

    coup_copy.wait()
    table_copy.wait()
    for d in range(1, lanes):
        map_sends[d - 1].wait_send()
    pltpu.make_async_copy(others, others, rm_send).wait()
    for copies in (z_copies, f_copies, p_copies):
        for copy in copies.values():
            copy.wait_send()
    for c in range(n_chunks):
        for h in range(2):
            own_copy(c, h).wait()
            sent = seconds[c].at[h, pl.ds(4, 28)]
            pltpu.make_async_copy(sent, sent, x_send.at[c, h]).wait()
            pltpu.make_async_copy(sent, sent, x_recv.at[c, h]).wait()


def assemble(
    owners, table_hbm, recv0_hbm, recv1_hbm, coup_hbm, k_hbm, m_hbm, coup_out,
    table, buf0, buf1, k_acc, m_acc, coup, table_sem, in_sem, out_sem, coup_in, coup_back,
):
    me = lax.axis_index("row")
    pairs = len(PAIRS)
    half = buf0.shape[2]
    to_scalars = pltpu.make_async_copy(table_hbm, table, table_sem)
    to_scalars.start()

    def begin(mat):
        def one(q, carry):
            plane = mat * pairs + q
            for src, dst, h in ((recv0_hbm, buf0, 0), (recv1_hbm, buf1, 1)):
                pltpu.make_async_copy(src.at[plane], dst.at[plane], in_sem.at[mat, h]).start()
            return carry

        lax.fori_loop(0, pairs, one, 0)

    def ready(mat):
        planes = pl.ds(mat * pairs, pairs)
        for src, dst, h in ((recv0_hbm, buf0, 0), (recv1_hbm, buf1, 1)):
            pltpu.make_async_copy(src.at[planes], dst.at[planes], in_sem.at[mat, h]).wait()

    begin(0)
    begin(1)
    take = pltpu.make_async_copy(coup_hbm, coup, coup_in)
    take.start()

    def clear(e, carry):
        k_acc[e] = jnp.zeros(k_acc.shape[1:], jnp.float32)
        m_acc[e] = jnp.zeros(m_acc.shape[1:], jnp.float32)
        return carry

    lax.fori_loop(0, BPO * BAND + 1, clear, 0)
    to_scalars.wait()

    def add(acc, mat):
        def one(y, carry):
            for g in range(4):
                for k in range(2):
                    r = y * 8 + g * 2 + k
                    spots = ((g * 2 + k) * 4 + (me // 8 + 4 - y) % 4, (y * 2 + k) * 4 + (me // 2 + 4 - g) % 4)
                    entries = [table[r, 0, p] for p in range(pairs)]
                    sums = [
                        acc[e, h * half:(h + 1) * half, :] + buf[mat * pairs + p, spots[h]]
                        for p, e in enumerate(entries) for h, buf in enumerate((buf0, buf1))
                    ]
                    for i, total in enumerate(sums):
                        h = i % 2
                        acc[entries[i // 2], h * half:(h + 1) * half, :] = total
            return carry

        lax.fori_loop(0, 4, one, 0)

    ready(0)
    add(k_acc, 0)
    k_out = pltpu.make_async_copy(k_acc.at[pl.ds(0, BPO * BAND)], k_hbm, out_sem.at[0])
    k_out.start()
    take.wait()
    give = pltpu.make_async_copy(coup, coup_out, coup_back)
    give.start()
    ready(1)
    add(m_acc, 1)
    m_out = pltpu.make_async_copy(m_acc.at[pl.ds(0, BPO * BAND)], m_hbm, out_sem.at[1])
    m_out.start()
    k_out.wait()
    give.wait()
    m_out.wait()


def per_device(stiff_bb, stiff_bi, constraint_modes, interior_mass, fixed_modes, mass_bb, boundary_map):
    owners, lanes = lax.axis_size("row"), lax.axis_size("col")
    count, inner, order = constraint_modes.shape
    modes = fixed_modes.shape[2]
    width = order // 3
    part = width // lanes
    half = part // 2
    group = lanes * count
    planes = 2 * len(PAIRS)

    anywhere = pl.BlockSpec(memory_space=pl.ANY)
    f32, bf16, i32 = jnp.float32, jnp.bfloat16, jnp.int32
    dma = pltpu.SemaphoreType.DMA
    received0, received1, table, coupling = pl.pallas_call(
        functools.partial(reduce_and_send, owners, lanes),
        out_shape=(
            jax.ShapeDtypeStruct((planes, owners, half, width), f32),
            jax.ShapeDtypeStruct((planes, owners, half, width), f32),
            jax.ShapeDtypeStruct((owners, 1, 128), i32),
            jax.ShapeDtypeStruct((count, modes, order), f32),
        ),
        in_specs=[anywhere] * 7,
        out_specs=(anywhere,) * 4,
        scratch_shapes=[
            pltpu.VMEM((count, inner, order), bf16),
            pltpu.VMEM((count, order, inner), bf16),
            pltpu.VMEM((count, inner, modes), bf16),
            pltpu.VMEM((count, inner, order), bf16),
            pltpu.VMEM((count, 3, width, order), bf16),
            pltpu.VMEM((count, 3, width, order), bf16),
            pltpu.VMEM((count, inner), f32),
            pltpu.VMEM((count, 128, 128), f32),
            pltpu.VMEM((count, modes, order), f32),
            pltpu.SMEM((count, 3), i32),
            pltpu.VMEM((1, 1, 128), i32),
            pltpu.VMEM((lanes, 1, 128), i32),
            pltpu.VMEM((1, 1, 128), i32),
            pltpu.SMEM((1, 1, 128), i32),
            pltpu.VMEM((owners, 1, 128), i32),
            pltpu.SMEM((owners, 1, 128), i32),
            pltpu.SMEM((32,), i32),
            pltpu.SMEM((64,), i32),
            pltpu.VMEM((owners, 1, 128), i32),
        ]
        + [pltpu.VMEM((count, 3 - b, width, width), f32) for _, b in BLOCKS]
        + [pltpu.VMEM((group, 2, half, width), f32)] * len(CHUNKS)
        + [pltpu.VMEM((2, 16, half, width), f32)] * len(CHUNKS)
        + [pltpu.VMEM((2, 24, half, width), f32)] * len(CHUNKS)
        + [pltpu.VMEM((2, 32, half, width), f32)] * len(CHUNKS)
        + [
            dma((13,)), dma, dma, dma((lanes - 1,)), dma((lanes - 1,)), dma, dma, dma, dma,
            dma((len(CHUNKS), 2, lanes - 1)), dma((len(CHUNKS), 2, lanes - 1)),
            dma((len(CHUNKS), 2, 2)), dma((len(CHUNKS), 2, 2)), dma((len(CHUNKS), 2, 2)), dma((len(CHUNKS), 2, 2)),
            dma((len(CHUNKS), 2)), dma((len(CHUNKS), 2)), dma((len(CHUNKS), 2)),
        ],
        compiler_params=pltpu.CompilerParams(
            collective_id=0, has_side_effects=True, vmem_limit_bytes=60 * 1024 * 1024),
        name="reduce_and_send",
    )(boundary_map, interior_mass, stiff_bb, stiff_bi, constraint_modes, fixed_modes, mass_bb)

    entry = (BPO * BAND, part, width)
    in_hbm = pl.BlockSpec(memory_space=pltpu.HBM)
    k_band, m_band, coupling = pl.pallas_call(
        functools.partial(assemble, owners),
        out_shape=(
            jax.ShapeDtypeStruct(entry, f32),
            jax.ShapeDtypeStruct(entry, f32),
            jax.ShapeDtypeStruct((count, modes, order), f32),
        ),
        in_specs=[in_hbm] * 4,
        out_specs=[in_hbm] * 3,
        scratch_shapes=[
            pltpu.SMEM((owners, 1, 128), i32),
            pltpu.VMEM((planes, owners, half, width), f32),
            pltpu.VMEM((planes, owners, half, width), f32),
            pltpu.VMEM((BPO * BAND + 1, part, width), f32),
            pltpu.VMEM((BPO * BAND + 1, part, width), f32),
            pltpu.VMEM((count, modes, order), f32),
            dma, dma((2, 2)), dma((2,)), dma, dma,
        ],
        compiler_params=pltpu.CompilerParams(vmem_limit_bytes=60 * 1024 * 1024),
        name="assemble",
    )(table, received0, received1, coupling)
    banded = (BPO, BAND, part, width)
    return k_band.reshape(banded), m_band.reshape(banded), coupling


def solution(mesh):
    both = ("row", "col")
    return jax.shard_map(
        per_device,
        mesh=mesh,
        in_specs=(
            P(both, None, None, None), P(both, None, None), P(both, None, None), P(both, None),
            P(both, None, None), P(both, None, None, None), P(both, None),
        ),
        out_specs=(P("row", None, "col", None), P("row", None, "col", None), P(both, None, None)),
        check_vma=False,
    )
```
